128 devices in a mesh: tm: 4 (over x), rows: 8 (over y, core), batch: 4 (over z).
Axes of the slice: x: 4, y: 4, z: 4, core: 2. Of those that a mesh axis runs over, the one named last changes fastest.
Arguments:
- inputs: bfloat16 [4, 8, 64, 128, 384], P('batch', 'tm', 'rows'), parts along dimension 0, may hold values from -16 to 16
- norm_gain: float32 [384], replicated, may hold values from 0.1 to 1.9
- norm_bias: float32 [384], replicated, may hold values from -3 to 3
- conv_weight: bfloat16 [3, 3, 3, 384, 384], replicated, may hold values from -0.0625 to 0.0625
- conv_bias: float32 [384], replicated, may hold values from -2 to 2
Outputs:
- decoded: bfloat16 [4, 8, 64, 128, 384], P('batch', 'tm', 'rows'), parts along dimension 0
The draws below stay inside these ranges and needn't reach their ends.
There are 4 independent parts, one for each index of `batch`. The reference program is written for one: setup_inputs(seed, part) draws one part's arguments, and reference() takes and returns one part's arrays. A program takes and returns all parts, laid end to end along the dimension named above; an argument that names none is the same for every part. Nothing has to cross between parts.
All inputs are finite; a program needn't handle non-finite values.
Results may differ from the reference program's by a relative error of at most 0.0025.
Values may be sent and summed in bfloat16 or wider, within the bound.
A program may use at most 128 MiB of HBM per device.

```python
import jax
import jax.numpy as jnp
from jax import lax

CHANNELS = 384
GROUPS = 32
WIDTH = 128
CLIPS = 1
FRAMES = 8
HEIGHT = 64


def draw_inputs(key, part):
    subkeys = jax.random.split(jax.random.fold_in(key, 17), 4)
    full_shape = (CLIPS, FRAMES, HEIGHT, WIDTH, CHANNELS)
    scales = 0.6 * jnp.exp(jax.random.uniform(subkeys[0], (CLIPS, FRAMES, HEIGHT, 1, 1), jnp.float32, -1.2, 1.2))
    offsets = 1.2 + 0.4 * jax.random.truncated_normal(subkeys[1], -5.0, 5.0, (CHANNELS,), jnp.float32)
    row_place = (jnp.arange(HEIGHT, dtype=jnp.float32) + 0.5) / HEIGHT
    row_ramp = (3.0 * row_place - 1.5).reshape(1, 1, HEIGHT, 1, 1)
    frame_level = jax.random.uniform(subkeys[3], (CLIPS, FRAMES, 1, 1, 1), jnp.float32, -1.2, 1.2)
    region = row_ramp + frame_level
    noisy_part = jax.random.truncated_normal(subkeys[2], -4.0, 4.0, full_shape, jnp.float32)
    values = noisy_part * scales + offsets + region
    return values.astype(jnp.bfloat16)


def bell_draw(key, extent, scale, limit, kind=jnp.bfloat16):
    values = jax.random.normal(key, extent, jnp.float32) * scale
    return jnp.minimum(jnp.maximum(values, -limit), limit).astype(kind)


def setup_inputs(seed: int = 0, part: int = 0) -> dict:
    key_list = jax.random.split(jax.random.key(seed), 6)
    own_keys = jax.random.split(jax.random.fold_in(key_list[5], part), 6)
    return {
        "inputs": draw_inputs(jax.random.fold_in(jax.random.fold_in(key_list[5], part), 71), part),
        "norm_gain": jnp.clip(1.0 + 0.18 * jax.random.normal(key_list[1], (CHANNELS,), jnp.float32), 0.1, 1.9),
        "norm_bias": bell_draw(key_list[2], (CHANNELS,), 0.5, 3.0, jnp.float32),
        "conv_weight": bell_draw(key_list[3], (3, 3, 3, CHANNELS, CHANNELS), (27 * CHANNELS) ** -0.5, 0.0625),
        "conv_bias": bell_draw(key_list[4], (CHANNELS,), 0.3, 2.0, jnp.float32),
    }


epsilon = 1e-06

def convolve(padded, conv_weight, frames, height, width):
    channels = padded.shape[-1]
    summed = jnp.zeros((padded.shape[0] * frames * height * width, conv_weight.shape[-1]), jnp.float32)
    for tap_time in range(3):
        for tap_row in range(3):
            slab_rows = padded[:, tap_time:tap_time + frames, tap_row:tap_row + height]
            columns = jnp.concatenate([slab_rows[:, :, :, 0:width], slab_rows[:, :, :, 1:width + 1], slab_rows[:, :, :, 2:width + 2]], axis=-1)
            kernel = conv_weight[tap_time, tap_row].reshape(3 * channels, -1)
            summed = summed + jnp.dot(columns.reshape(-1, 3 * channels), kernel, preferred_element_type=jnp.float32)
    return summed

def reference(inputs, norm_gain, norm_bias, conv_weight, conv_bias):
    values = inputs.astype(jnp.float32)
    channels = values.shape[-1]
    per_group = channels // GROUPS
    cell_count = 1.0 * CLIPS * FRAMES * HEIGHT * WIDTH * per_group
    chan_sum = lax.optimization_barrier(jnp.sum(values, axis=(0, 1, 2, 3)))
    group_mean = lax.optimization_barrier(jnp.sum(chan_sum.reshape(GROUPS, per_group), axis=1)) / cell_count
    centered = values - jnp.repeat(group_mean, per_group)
    chan_square = lax.optimization_barrier(jnp.sum(centered * centered, axis=(0, 1, 2, 3)))
    group_var = lax.optimization_barrier(jnp.sum(chan_square.reshape(GROUPS, per_group), axis=1)) / cell_count
    inverse = jnp.repeat(lax.rsqrt(group_var + epsilon), per_group)
    normed = centered * inverse * norm_gain + norm_bias
    active = (normed * jax.nn.sigmoid(normed)).astype(jnp.bfloat16)
    padded = jnp.pad(active, ((0, 0), (2, 0), (1, 1), (1, 1), (0, 0)))
    summed = convolve(padded, conv_weight, FRAMES, HEIGHT, WIDTH)
    result = values + summed.reshape(values.shape) + conv_bias
    return result.astype(jnp.bfloat16)
```

```python
import functools

import jax
import jax.numpy as jnp
from jax import lax
from jax.experimental import pallas as pl
from jax.experimental.pallas import tpu as pltpu
from jax.sharding import PartitionSpec as P

MESH = pl.DeviceIdType.MESH
GROUPS = 32
EPS = 1e-06
F32 = jnp.float32
BF16 = jnp.bfloat16

PIECES = ((1, 0, 1), (1, 7, 1), (1, 1, 3), (1, 4, 3), (0, 0, 1), (0, 7, 1), (0, 1, 4), (0, 5, 2))


def kernel(
    cells, per_group,
    x, gain, bias, cbias, w, out,
    xo, xr, act, wv, z, ost, ind, tm_out, tm_in, row_out, row_in,
    load_sem, wsem, out_sem,
    bulk_send, bulk_recv, halo_send, halo_recv, fwd_send, fwd_recv,
    tm_send, tm_recv, row_send, row_recv,
):
    n_tm, n_rows = lax.axis_size("tm"), lax.axis_size("rows")
    j, r = lax.axis_index("tm"), lax.axis_index("rows")
    frames, height, width, ch = xo.shape[0], xo.shape[1] - 2, xo.shape[2], xo.shape[3]

    load = pltpu.make_async_copy(x.at[0], xo.at[:, 1 : height + 1], load_sem)
    load.start()
    wloads = [
        pltpu.make_async_copy(w.at[:, :, kw], wv.at[:, :, :, pl.ds(kw * ch, ch)], wsem.at[kw])
        for kw in range(3)
    ]
    for c in wloads:
        c.start()

    barrier = pltpu.get_barrier_semaphore()
    tm_peers = [{"tm": lax.rem(j + d, n_tm)} for d in range(1, n_tm)]
    row_peers = [{"rows": lax.rem(r + d, n_rows)} for d in range(1, n_rows)]
    for peer in tm_peers + row_peers:
        pl.semaphore_signal(barrier, inc=1, device_id=peer, device_id_type=MESH)
    pl.semaphore_wait(barrier, len(tm_peers) + len(row_peers))

    def bulk(i):
        f, first, rows = PIECES[i]
        return pltpu.make_async_remote_copy(
            src_ref=x.at[0, f, pl.ds(first, rows)],
            dst_ref=xr.at[f, pl.ds(1 + first, rows)],
            send_sem=bulk_send.at[i],
            recv_sem=bulk_recv.at[i],
            device_id={"tm": lax.rem(j + 1, n_tm)},
            device_id_type=MESH,
        )

    def edge(i, src, dst, ssem, rsem):
        return pltpu.make_async_remote_copy(
            src_ref=src, dst_ref=dst, send_sem=ssem, recv_sem=rsem,
            device_id={"rows": lax.rem(r + (n_rows - 1 if i == 0 else 1), n_rows)},
            device_id_type=MESH,
        )

    def own_edge(i):
        return edge(
            i, x.at[0, :, 0 if i == 0 else height - 1], xo.at[:, height + 1 if i == 0 else 0],
            halo_send.at[i], halo_recv.at[i],
        )

    def fwd_edge(f, i):
        return edge(
            i, xr.at[f, 1 if i == 0 else height], xr.at[f, height + 1 if i == 0 else 0],
            fwd_send.at[2 * f + i], fwd_recv.at[2 * f + i],
        )

    sends_on, recvs_on = j < n_tm - 1, j > 0
    up_on, down_on = r > 0, r < n_rows - 1

    @pl.when(sends_on)
    def _():
        bulk(0).start()
        bulk(1).start()

    @pl.when(up_on)
    def _():
        own_edge(0).start()

    @pl.when(down_on)
    def _():
        own_edge(1).start()

    a = lax.broadcasted_iota(jnp.int32, (ch, ch), 0)
    b = lax.broadcasted_iota(jnp.int32, (ch, ch), 1)
    group_of = lambda i: lax.shift_right_logical(i * 43691, 19)
    ind[...] = jnp.where(group_of(a) == group_of(b), 1.0, 0.0).astype(BF16)

    def over_group(v):
        hi = v.astype(BF16).astype(F32)
        mid = (v - hi).astype(BF16).astype(F32)
        lo = v - hi - mid
        parts = jnp.concatenate([hi, mid, lo, jnp.zeros_like(v)], axis=0).astype(BF16)
        got = jnp.dot(parts, ind[...], preferred_element_type=F32)
        return got[0:8] + (got[8:16] + got[16:24])

    load.wait()
    local = 1.0 * frames * height * width * per_group

    def fold(v):
        return jnp.sum(v.reshape(-1, 8, ch), axis=0)

    def all_rows(v):
        return jnp.broadcast_to(jnp.sum(v, axis=0, keepdims=True), (8, ch))

    def sum_body(i, acc):
        v = xo[lax.div(i, height), 1 + lax.rem(i, height)].astype(F32)
        return acc + fold(v)

    total = lax.fori_loop(0, frames * height, sum_body, jnp.zeros((8, ch), F32))
    mean = over_group(all_rows(total)) * (1.0 / local)

    def square_body(i, acc):
        v = xo[lax.div(i, height), 1 + lax.rem(i, height)].astype(F32)
        d = v - mean[0:1]
        return acc + fold(d * d)

    total = lax.fori_loop(0, frames * height, square_body, jnp.zeros((8, ch), F32))
    square = over_group(all_rows(total))

    top = lax.broadcasted_iota(jnp.int32, (8, ch), 0) == 0

    def exchange(mean, square, count, axis, peers, index, outbox, inbox, ssem, rsem):
        size = len(peers) + 1
        outbox[...] = jnp.where(top, mean, square)
        copies = [
            pltpu.make_async_remote_copy(
                src_ref=outbox, dst_ref=inbox.at[d], send_sem=ssem.at[d], recv_sem=rsem.at[d],
                device_id=peers[d], device_id_type=MESH,
            )
            for d in range(size - 1)
        ]
        for c in copies:
            c.start()
        for c in copies:
            c.wait()
        got = [inbox[d] for d in range(size - 1)]
        means = [mean[0:1]] + [g[0:1] for g in got]
        whole = sum(means) * (1.0 / size)
        squares = square[0:1] + sum(g[1:2] for g in got)
        for m in means:
            squares = squares + count * ((m - whole) * (m - whole))
        return jnp.broadcast_to(whole, (8, ch)), jnp.broadcast_to(squares, (8, ch))

    mean, square = exchange(mean, square, local, "tm", tm_peers, j, tm_out, tm_in, tm_send, tm_recv)

    @pl.when(sends_on)
    def _():
        for i in range(2, len(PIECES)):
            bulk(i).start()

    mean, square = exchange(
        mean, square, local * n_tm, "rows", row_peers, r, row_out, row_in, row_send, row_recv
    )
    inverse = lax.rsqrt(square[0:1] * (1.0 / cells) + EPS)
    mean = mean[0:1]
    scale = 0.5 * (inverse * gain[...])
    shift = 0.5 * bias[...]

    def activate(v):
        h = (v.astype(F32) - mean) * scale + shift
        return (h + h * jnp.tanh(h)).astype(BF16)

    def normalize(src, f, dst, first, count):
        def body(i, _):
            act[dst, first + i] = activate(src[f, first + i])
            return 0

        lax.fori_loop(0, count, body, 0)

    def normalize_edges(src, f, dst):
        for on, row in ((up_on, 0), (down_on, height + 1)):

            @pl.when(on)
            def _():
                act[dst, row] = activate(src[f, row])

            @pl.when(jnp.logical_not(on))
            def _():
                act[dst, row] = jnp.zeros((width, ch), BF16)

    def product(t, used, kt, first, rows, add):
        m, k = rows * width, 3 * ch
        lhs = jnp.concatenate(
            [act[f, pl.ds(first + kh, rows)].reshape(m, ch) for f in used for kh in range(3)], axis=1
        )
        for lo in range(0, 3 * ch, 256):
            n = min(256, 3 * ch - lo)
            rhs = wv[pl.ds(kt, len(used)), :, :, pl.ds(lo, n)].reshape(len(used) * k, n)
            got = jnp.dot(lhs, rhs, preferred_element_type=F32).reshape(rows, width, n)
            at = (t, pl.ds(first, rows), slice(None), pl.ds(lo, n))
            z[at] = z[at] + got if add else got

    wi = lax.broadcasted_iota(jnp.int32, (width, ch), 0)

    def finish(t, first, rows):
        def body(i, _):
            h = first + i
            left = pltpu.roll(z[t, h, :, 0:ch], 1, 0)
            right = pltpu.roll(z[t, h, :, 2 * ch : 3 * ch], width - 1, 0)
            conv = z[t, h, :, ch : 2 * ch]
            conv = conv + jnp.where(wi == 0, 0.0, left) + jnp.where(wi == width - 1, 0.0, right)
            ost[t, h] = (xo[t, h + 1].astype(F32) + conv + cbias[...]).astype(BF16)
            return 0

        lax.fori_loop(0, rows, body, 0)

    def output(t, first, rows, i):
        return pltpu.make_async_copy(
            ost.at[t, pl.ds(first, rows)], out.at[0, t, pl.ds(first, rows)], out_sem.at[i]
        )

    for f in range(frames):
        normalize(xo, f, 2 + f, 1, height)

    @pl.when(down_on)
    def _():
        own_edge(0).wait_recv()

    @pl.when(up_on)
    def _():
        own_edge(1).wait_recv()

    for f in range(frames):
        normalize_edges(xo, f, 2 + f)

    def forward(f):
        @pl.when(recvs_on)
        def _():
            a, b = [i for i, p in enumerate(PIECES) if p[0] == f][:2]
            bulk(a).wait_recv()
            bulk(b).wait_recv()

            @pl.when(up_on)
            def _():
                fwd_edge(f, 0).start()

            @pl.when(down_on)
            def _():
                fwd_edge(f, 1).start()

    forward(1)
    for c in wloads:
        c.wait()

    half = height // 2

    @pl.loop(0, 2)
    def _(i):
        product(0, (2,), 2, i * half, half, False)
        product(1, (2, 3), 1, i * half, half, False)

    def edges_in(f):
        @pl.when(down_on)
        def _():
            fwd_edge(f, 0).wait_recv()

        @pl.when(up_on)
        def _():
            fwd_edge(f, 1).wait_recv()

    forward(0)

    @pl.when(recvs_on)
    def _():
        edges_in(1)
        for i in (2, 3):
            bulk(i).wait_recv()
        normalize(xr, 1, 1, 1, height)
        normalize_edges(xr, 1, 1)

        @pl.loop(0, 2)
        def _(i):
            product(0, (1,), 1, i * half, half, True)
            product(1, (1,), 0, i * half, half, True)

    finish(1, 0, height)
    output(1, 0, height, 0).start()

    @pl.when(recvs_on)
    def _():
        edges_in(0)
        normalize_edges(xr, 0, 0)
        bulk(6).wait_recv()
        normalize(xr, 0, 0, 1, 5)
        normalize(xr, 0, 0, 8, 1)
        product(0, (0,), 0, 0, half, True)

    finish(0, 0, half)
    output(0, 0, half, 1).start()

    @pl.when(recvs_on)
    def _():
        bulk(7).wait_recv()
        normalize(xr, 0, 0, 6, 2)
        product(0, (0,), 0, half, half, True)

    finish(0, half, half)
    output(0, half, half, 2).start()

    @pl.when(sends_on)
    def _():
        for i in range(len(PIECES)):
            bulk(i).wait_send()

    for i, on in ((0, up_on), (1, down_on)):

        @pl.when(on)
        def _():
            own_edge(i).wait_send()

            @pl.when(recvs_on)
            def _():
                for f in range(2):
                    fwd_edge(f, i).wait_send()

    output(1, 0, height, 0).wait()
    output(0, 0, half, 1).wait()
    output(0, half, half, 2).wait()


def shards(inputs, norm_gain, norm_bias, conv_weight, conv_bias):
    clips, frames, height, width, ch = inputs.shape
    n_tm, n_rows = lax.axis_size("tm"), lax.axis_size("rows")
    per_group = ch // GROUPS
    cells = 1.0 * clips * frames * height * width * per_group * n_tm * n_rows
    any_space = pl.BlockSpec(memory_space=pl.ANY)
    vmem = pl.BlockSpec(memory_space=pltpu.VMEM)
    dma = lambda n: pltpu.SemaphoreType.DMA((n,))
    return pl.pallas_call(
        functools.partial(kernel, cells, per_group),
        out_shape=jax.ShapeDtypeStruct(inputs.shape, BF16),
        in_specs=[any_space, vmem, vmem, vmem, any_space],
        out_specs=any_space,
        scratch_shapes=[
            pltpu.VMEM((frames, height + 2, width, ch), BF16),
            pltpu.VMEM((2, height + 2, width, ch), BF16),
            pltpu.VMEM((frames + 2, height + 2, width, ch), BF16),
            pltpu.VMEM((3, 3, ch, 3 * ch), BF16),
            pltpu.VMEM((frames, height, width, 3 * ch), F32),
            pltpu.VMEM((frames, height, width, ch), BF16),
            pltpu.VMEM((ch, ch), BF16),
            pltpu.VMEM((8, ch), F32),
            pltpu.VMEM((n_tm - 1, 8, ch), F32),
            pltpu.VMEM((8, ch), F32),
            pltpu.VMEM((n_rows - 1, 8, ch), F32),
            pltpu.SemaphoreType.DMA,
            dma(3),
            dma(3),
            dma(len(PIECES)),
            dma(len(PIECES)),
            dma(2),
            dma(2),
            dma(4),
            dma(4),
            dma(n_tm - 1),
            dma(n_tm - 1),
            dma(n_rows - 1),
            dma(n_rows - 1),
        ],
        compiler_params=pltpu.CompilerParams(
            collective_id=0, has_side_effects=True, vmem_limit_bytes=60 * 1024 * 1024
        ),
    )(
        inputs,
        norm_gain.reshape(1, ch),
        norm_bias.reshape(1, ch),
        conv_bias.reshape(1, ch),
        conv_weight,
    )


def solution(mesh):
    placed = (P("batch", "tm", "rows", None, None), P(), P(), P(), P())
    return jax.shard_map(
        shards,
        mesh=mesh,
        in_specs=placed,
        out_specs=P("batch", "tm", "rows", None, None),
        check_vma=False,
    )
```

```python
import functools

import jax
import jax.numpy as jnp
from jax import lax
from jax.experimental import pallas as pl
from jax.experimental.pallas import tpu as pltpu
from jax.sharding import PartitionSpec as P

MESH = pl.DeviceIdType.MESH
GROUPS = 32
EPS = 1e-06
F32 = jnp.float32
BF16 = jnp.bfloat16

PIECES = ((1, 0, 1), (1, 7, 1), (1, 1, 3), (1, 4, 3), (0, 0, 1), (0, 7, 1), (0, 1, 4), (0, 5, 2))


def kernel(
    cells, per_group,
    x, vec, w, out,
    xo, xr, act, wv, z, ost, ind, tm_out, tm_in, row_out, row_in,
    gv, load_sem, wsem, out_sem, vec_sem,
    bulk_send, bulk_recv, halo_send, halo_recv, fwd_send, fwd_recv,
    tm_send, tm_recv, row_send, row_recv,
):
    n_tm, n_rows = lax.axis_size("tm"), lax.axis_size("rows")
    j, r = lax.axis_index("tm"), lax.axis_index("rows")
    frames, height, width, ch = xo.shape[0], xo.shape[1] - 2, xo.shape[2], xo.shape[3]

    load = pltpu.make_async_copy(x.at[0], xo.at[:, 1 : height + 1], load_sem)
    load.start()
    wloads = [
        pltpu.make_async_copy(w.at[:, :, kw], wv.at[:, :, :, pl.ds(kw * ch, ch)], wsem.at[kw])
        for kw in range(3)
    ]
    for c in wloads:
        c.start()
    vectors = [pltpu.make_async_copy(vec, gv, vec_sem)]
    for c in vectors:
        c.start()

    barrier = pltpu.get_barrier_semaphore()
    tm_peers = [{"tm": lax.rem(j + d, n_tm)} for d in range(1, n_tm)]
    row_peers = [{"rows": lax.rem(r + d, n_rows)} for d in range(1, n_rows)]
    for peer in tm_peers + row_peers:
        pl.semaphore_signal(barrier, inc=1, device_id=peer, device_id_type=MESH)
    pl.semaphore_wait(barrier, len(tm_peers) + len(row_peers))

    def bulk(i):
        f, first, rows = PIECES[i]
        return pltpu.make_async_remote_copy(
            src_ref=x.at[0, f, pl.ds(first, rows)],
            dst_ref=xr.at[f, pl.ds(1 + first, rows)],
            send_sem=bulk_send.at[i],
            recv_sem=bulk_recv.at[i],
            device_id={"tm": lax.rem(j + 1, n_tm)},
            device_id_type=MESH,
        )

    def edge(i, src, dst, ssem, rsem):
        return pltpu.make_async_remote_copy(
            src_ref=src, dst_ref=dst, send_sem=ssem, recv_sem=rsem,
            device_id={"rows": lax.rem(r + (n_rows - 1 if i == 0 else 1), n_rows)},
            device_id_type=MESH,
        )

    def own_edge(i):
        return edge(
            i, x.at[0, :, 0 if i == 0 else height - 1], xo.at[:, height + 1 if i == 0 else 0],
            halo_send.at[i], halo_recv.at[i],
        )

    def fwd_edge(f, i):
        return edge(
            i, xr.at[f, 1 if i == 0 else height], xr.at[f, height + 1 if i == 0 else 0],
            fwd_send.at[2 * f + i], fwd_recv.at[2 * f + i],
        )

    sends_on, recvs_on = j < n_tm - 1, j > 0
    up_on, down_on = r > 0, r < n_rows - 1

    @pl.when(sends_on)
    def _():
        bulk(0).start()
        bulk(1).start()

    @pl.when(up_on)
    def _():
        own_edge(0).start()

    @pl.when(down_on)
    def _():
        own_edge(1).start()

    a = lax.broadcasted_iota(jnp.int32, (ch, ch), 0)
    b = lax.broadcasted_iota(jnp.int32, (ch, ch), 1)
    group_of = lambda i: lax.shift_right_logical(i * 43691, 19)
    ind[...] = jnp.where(group_of(a) == group_of(b), 1.0, 0.0).astype(BF16)

    def over_group(v):
        hi = v.astype(BF16).astype(F32)
        mid = (v - hi).astype(BF16).astype(F32)
        lo = v - hi - mid
        parts = jnp.concatenate([hi, mid, lo, jnp.zeros_like(v)], axis=0).astype(BF16)
        got = jnp.dot(parts, ind[...], preferred_element_type=F32)
        return got[0:8] + (got[8:16] + got[16:24])

    load.wait()
    for c in vectors:
        c.wait()
    local = 1.0 * frames * height * width * per_group

    def fold(v):
        return jnp.sum(v.reshape(-1, 8, ch), axis=0)

    def all_rows(v):
        return jnp.broadcast_to(jnp.sum(v, axis=0, keepdims=True), (8, ch))

    def sum_body(i, acc):
        v = xo[lax.div(i, height), 1 + lax.rem(i, height)].astype(F32)
        return acc + fold(v)

    total = lax.fori_loop(0, frames * height, sum_body, jnp.zeros((8, ch), F32))
    mean = over_group(all_rows(total)) * (1.0 / local)

    def square_body(i, acc):
        v = xo[lax.div(i, height), 1 + lax.rem(i, height)].astype(F32)
        d = v - mean[0:1]
        return acc + fold(d * d)

    total = lax.fori_loop(0, frames * height, square_body, jnp.zeros((8, ch), F32))
    square = over_group(all_rows(total))

    top = lax.broadcasted_iota(jnp.int32, (8, ch), 0) == 0

    def exchange(mean, square, count, peers, outbox, inbox, ssem, rsem, between):
        size = len(peers) + 1
        outbox[...] = jnp.where(top, mean, square)
        copies = [
            pltpu.make_async_remote_copy(
                src_ref=outbox, dst_ref=inbox.at[d], send_sem=ssem.at[d], recv_sem=rsem.at[d],
                device_id=peers[d], device_id_type=MESH,
            )
            for d in range(size - 1)
        ]
        for c in copies:
            c.start()
        between()
        for c in copies:
            c.wait()
        got = [inbox[d] for d in range(size - 1)]
        means = [mean[0:1]] + [g[0:1] for g in got]
        whole = sum(means) * (1.0 / size)
        squares = square[0:1] + sum(g[1:2] for g in got)
        for m in means:
            squares = squares + count * ((m - whole) * (m - whole))
        return jnp.broadcast_to(whole, (8, ch)), jnp.broadcast_to(squares, (8, ch))

    def rest_of_bulk():
        @pl.when(sends_on)
        def _():
            for i in range(2, len(PIECES)):
                bulk(i).start()

    mean, square = exchange(
        mean, square, local, tm_peers, tm_out, tm_in, tm_send, tm_recv, rest_of_bulk
    )
    mean, square = exchange(
        mean, square, local * n_tm, row_peers, row_out, row_in, row_send, row_recv, lambda: None
    )
    inverse = lax.rsqrt(square[0:1] * (1.0 / cells) + EPS)
    mean = mean[0:1]
    scale = 0.5 * (inverse * gv[pl.ds(0 * ch, ch)].reshape(1, ch))
    shift = 0.5 * gv[pl.ds(1 * ch, ch)].reshape(1, ch)

    def activate(v):
        h = (v.astype(F32) - mean) * scale + shift
        return (h + h * jnp.tanh(h)).astype(BF16)

    def normalize(src, f, dst, first, count):
        def body(i, _):
            act[dst, first + i] = activate(src[f, first + i])
            return 0

        lax.fori_loop(0, count, body, 0)

    def normalize_edges(src, f, dst):
        for on, row in ((up_on, 0), (down_on, height + 1)):

            @pl.when(on)
            def _():
                act[dst, row] = activate(src[f, row])

            @pl.when(jnp.logical_not(on))
            def _():
                act[dst, row] = jnp.zeros((width, ch), BF16)

    def product(t, used, kt, first, rows, add):
        m, k = rows * width, 3 * ch
        lhs = jnp.concatenate(
            [act[f, pl.ds(first + kh, rows)].reshape(m, ch) for f in used for kh in range(3)], axis=1
        )
        for lo in range(0, 3 * ch, 256):
            n = min(256, 3 * ch - lo)
            rhs = wv[pl.ds(kt, len(used)), :, :, pl.ds(lo, n)].reshape(len(used) * k, n)
            got = jnp.dot(lhs, rhs, preferred_element_type=F32).reshape(rows, width, n)
            at = (t, pl.ds(first, rows), slice(None), pl.ds(lo, n))
            z[at] = z[at] + got if add else got

    wi = lax.broadcasted_iota(jnp.int32, (width, ch), 0)

    def finish(t, first, rows):
        def body(i, _):
            h = first + i
            left = pltpu.roll(z[t, h, :, 0:ch], 1, 0)
            right = pltpu.roll(z[t, h, :, 2 * ch : 3 * ch], width - 1, 0)
            conv = z[t, h, :, ch : 2 * ch]
            conv = conv + jnp.where(wi == 0, 0.0, left) + jnp.where(wi == width - 1, 0.0, right)
            out[0, t, h] = (xo[t, h + 1].astype(F32) + conv + gv[pl.ds(2 * ch, ch)].reshape(1, ch)).astype(BF16)
            return 0

        lax.fori_loop(0, rows, body, 0)

    def output(t, first, rows, i):
        return pltpu.make_async_copy(
            ost.at[t, pl.ds(first, rows)], out.at[0, t, pl.ds(first, rows)], out_sem.at[i]
        )

    for f in range(frames):
        normalize(xo, f, 2 + f, 1, height)

    @pl.when(down_on)
    def _():
        own_edge(0).wait_recv()

    @pl.when(up_on)
    def _():
        own_edge(1).wait_recv()

    for f in range(frames):
        normalize_edges(xo, f, 2 + f)

    def forward(f):
        @pl.when(recvs_on)
        def _():
            a, b = [i for i, p in enumerate(PIECES) if p[0] == f][:2]
            bulk(a).wait_recv()
            bulk(b).wait_recv()

            @pl.when(up_on)
            def _():
                fwd_edge(f, 0).start()

            @pl.when(down_on)
            def _():
                fwd_edge(f, 1).start()

    forward(1)
    for c in wloads:
        c.wait()

    half = height // 2

    @pl.loop(0, 2)
    def _(i):
        product(0, (2,), 2, i * half, half, False)
        product(1, (2, 3), 1, i * half, half, False)

    def edges_in(f):
        @pl.when(down_on)
        def _():
            fwd_edge(f, 0).wait_recv()

        @pl.when(up_on)
        def _():
            fwd_edge(f, 1).wait_recv()

    forward(0)

    @pl.when(recvs_on)
    def _():
        edges_in(1)
        for i in (2, 3):
            bulk(i).wait_recv()
        normalize(xr, 1, 1, 1, height)
        normalize_edges(xr, 1, 1)

        @pl.loop(0, 2)
        def _(i):
            product(0, (1,), 1, i * half, half, True)
            product(1, (1,), 0, i * half, half, True)

    finish(1, 0, height)

    @pl.when(recvs_on)
    def _():
        edges_in(0)
        normalize_edges(xr, 0, 0)
        bulk(6).wait_recv()
        normalize(xr, 0, 0, 1, 5)
        normalize(xr, 0, 0, 8, 1)
        product(0, (0,), 0, 0, half, True)

    finish(0, 0, half)

    @pl.when(recvs_on)
    def _():
        bulk(7).wait_recv()
        normalize(xr, 0, 0, 6, 2)
        product(0, (0,), 0, half, half, True)

    finish(0, half, half)

    @pl.when(sends_on)
    def _():
        for i in range(len(PIECES)):
            bulk(i).wait_send()

    for i, on in ((0, up_on), (1, down_on)):

        @pl.when(on)
        def _():
            own_edge(i).wait_send()

            @pl.when(recvs_on)
            def _():
                for f in range(2):
                    fwd_edge(f, i).wait_send()


def shards(inputs, norm_gain, norm_bias, conv_weight, conv_bias):
    clips, frames, height, width, ch = inputs.shape
    n_tm, n_rows = lax.axis_size("tm"), lax.axis_size("rows")
    per_group = ch // GROUPS
    cells = 1.0 * clips * frames * height * width * per_group * n_tm * n_rows
    any_space = pl.BlockSpec(memory_space=pltpu.HBM)
    dma = lambda n: pltpu.SemaphoreType.DMA((n,))
    return pl.pallas_call(
        functools.partial(kernel, cells, per_group),
        out_shape=jax.ShapeDtypeStruct(inputs.shape, BF16),
        in_specs=[any_space] * 3,
        out_specs=pl.BlockSpec(memory_space=pltpu.VMEM),
        scratch_shapes=[
            pltpu.VMEM((frames, height + 2, width, ch), BF16),
            pltpu.VMEM((2, height + 2, width, ch), BF16),
            pltpu.VMEM((frames + 2, height + 2, width, ch), BF16),
            pltpu.VMEM((3, 3, ch, 3 * ch), BF16),
            pltpu.VMEM((frames, height, width, 3 * ch), F32),
            pltpu.VMEM((frames, height, width, ch), BF16),
            pltpu.VMEM((ch, ch), BF16),
            pltpu.VMEM((8, ch), F32),
            pltpu.VMEM((n_tm - 1, 8, ch), F32),
            pltpu.VMEM((8, ch), F32),
            pltpu.VMEM((n_rows - 1, 8, ch), F32),
            pltpu.VMEM((3 * ch,), F32),
            pltpu.SemaphoreType.DMA,
            dma(3),
            dma(3),
            pltpu.SemaphoreType.DMA,
            dma(len(PIECES)),
            dma(len(PIECES)),
            dma(2),
            dma(2),
            dma(4),
            dma(4),
            dma(n_tm - 1),
            dma(n_tm - 1),
            dma(n_rows - 1),
            dma(n_rows - 1),
        ],
        compiler_params=pltpu.CompilerParams(
            collective_id=0, has_side_effects=True, vmem_limit_bytes=51 * 1024 * 1024
        ),
    )(
        inputs,
        jnp.concatenate([norm_gain, norm_bias, conv_bias]),
        conv_weight,
    )


def solution(mesh):
    placed = (P("batch", "tm", "rows", None, None), P(), P(), P(), P())
    return jax.shard_map(
        shards,
        mesh=mesh,
        in_specs=placed,
        out_specs=P("batch", "tm", "rows", None, None),
        check_vma=False,
    )
```

```python
import functools

import jax
import jax.numpy as jnp
from jax import lax
from jax.experimental import pallas as pl
from jax.experimental.pallas import tpu as pltpu
from jax.sharding import PartitionSpec as P

MESH = pl.DeviceIdType.MESH
GROUPS = 32
EPS = 1e-06
F32 = jnp.float32
BF16 = jnp.bfloat16

PIECES = ((1, 0, 1), (1, 7, 1), (1, 1, 4), (1, 5, 2), (0, 0, 1), (0, 7, 1), (0, 1, 2), (0, 6, 1))
BACK = (3, 3)


def kernel(
    cells, per_group,
    x, vec, w, out,
    xo, xr, act_a, act_b, act_c, act_d, wv, z, ind, tm_out, tm_in, row_out, row_in, hop1, hop2, gv,
    load_sem, wsem, vec_sem,
    bulk_send, bulk_recv, back_send, back_recv, halo_send, halo_recv, fwd_send, fwd_recv,
    tm_send, tm_recv, row_send, row_recv,
):
    n_tm, n_rows = lax.axis_size("tm"), lax.axis_size("rows")
    j, r = lax.axis_index("tm"), lax.axis_index("rows")
    frames, height, width, ch = xo.shape[0], xo.shape[1] - 2, xo.shape[2], xo.shape[3]
    half = height // 2

    load = pltpu.make_async_copy(x.at[0], xo.at[:, 1 : height + 1], load_sem)
    load.start()
    vector = pltpu.make_async_copy(vec, gv, vec_sem)
    vector.start()
    wloads = [
        pltpu.make_async_copy(w.at[:, :, kw], wv.at[:, :, :, pl.ds(kw * ch, ch)], wsem.at[kw])
        for kw in range(3)
    ]
    for c in wloads:
        c.start()

    barrier = pltpu.get_barrier_semaphore()
    tm_peers = [{"tm": lax.rem(j + d, n_tm)} for d in range(1, n_tm)]
    row_peers = [{"rows": lax.rem(r + d, n_rows)} for d in range(1, n_rows)]
    for peer in tm_peers + row_peers:
        pl.semaphore_signal(barrier, inc=1, device_id=peer, device_id_type=MESH)

    def bulk(i):
        f, first, rows = PIECES[i]
        return pltpu.make_async_remote_copy(
            src_ref=x.at[0, f, pl.ds(first, rows)],
            dst_ref=xr.at[f, pl.ds(1 + first, rows)],
            send_sem=bulk_send.at[i],
            recv_sem=bulk_recv.at[i],
            device_id={"tm": lax.rem(j + 1, n_tm)},
            device_id_type=MESH,
        )

    def back(i):
        first, rows = BACK
        src, dst = (
            (x.at[0, 0, pl.ds(first, rows)], hop1),
            (hop1, hop2),
            (hop2, xr.at[0, pl.ds(1 + first, rows)]),
        )[i]
        return pltpu.make_async_remote_copy(
            src_ref=src, dst_ref=dst, send_sem=back_send.at[i], recv_sem=back_recv.at[i],
            device_id={"tm": lax.rem(j + n_tm - 1, n_tm)}, device_id_type=MESH,
        )

    def edge(i, src, dst, ssem, rsem):
        return pltpu.make_async_remote_copy(
            src_ref=src, dst_ref=dst, send_sem=ssem, recv_sem=rsem,
            device_id={"rows": lax.rem(r + (n_rows - 1 if i == 0 else 1), n_rows)},
            device_id_type=MESH,
        )

    def own_edge(i):
        return edge(
            i, x.at[0, :, 0 if i == 0 else height - 1], xo.at[:, height + 1 if i == 0 else 0],
            halo_send.at[i], halo_recv.at[i],
        )

    def fwd_edge(f, i):
        return edge(
            i, xr.at[f, 1 if i == 0 else height], xr.at[f, height + 1 if i == 0 else 0],
            fwd_send.at[2 * f + i], fwd_recv.at[2 * f + i],
        )

    sends_on, recvs_on = j < n_tm - 1, j > 0
    second_on, third_on = j != n_tm - 2, j != n_tm - 3
    up_on, down_on = r > 0, r < n_rows - 1

    @pl.when(jnp.logical_not(recvs_on))
    def _():
        xr[...] = jnp.zeros_like(xr)

    for on, row in ((up_on, 0), (down_on, height + 1)):

        @pl.when(jnp.logical_not(on))
        def _():
            xo[:, row] = jnp.zeros((frames, width, ch), BF16)
            xr[:, row] = jnp.zeros((2, width, ch), BF16)

    a = lax.broadcasted_iota(jnp.int32, (ch, ch), 0)
    b = lax.broadcasted_iota(jnp.int32, (ch, ch), 1)
    group_of = lambda i: lax.shift_right_logical(i * 43691, 19)
    ind[...] = jnp.where(group_of(a) == group_of(b), 1.0, 0.0).astype(BF16)

    def over_group(v):
        v = jnp.broadcast_to(v, (8, ch))
        hi = v.astype(BF16).astype(F32)
        mid = (v - hi).astype(BF16).astype(F32)
        lo = v - hi - mid
        parts = jnp.concatenate([hi, mid, lo, jnp.zeros_like(v)], axis=0).astype(BF16)
        got = jnp.dot(parts, ind[...], preferred_element_type=F32)
        return got[0:1] + (got[8:9] + got[16:17])

    load.wait()
    pixels = 1.0 * frames * height * width

    def fold(v):
        return jnp.sum(v.reshape(-1, 32, ch), axis=0)

    def over_rows(v):
        return jnp.sum(v, axis=0, keepdims=True)

    pivot = over_rows(fold(xo[0, 1].astype(F32))) * (1.0 / width)

    def sums(i, acc):
        first, second = acc
        d = xo[lax.div(i, height), 1 + lax.rem(i, height)].astype(F32) - pivot
        return first + fold(d), second + fold(d * d)

    zero = jnp.zeros((32, ch), F32)
    first, second = lax.fori_loop(0, frames * height, sums, (zero, zero))
    first, second = over_rows(first), over_rows(second)
    mean = pivot + first * (1.0 / pixels)
    square = second - first * (first * (1.0 / pixels))

    top = lax.broadcasted_iota(jnp.int32, (2, ch), 0) == 0

    def exchange(mean, square, count, peers, outbox, inbox, ssem, rsem, between):
        size = len(peers) + 1
        outbox[...] = jnp.where(top, mean, square)
        copies = [
            pltpu.make_async_remote_copy(
                src_ref=outbox, dst_ref=inbox.at[d], send_sem=ssem.at[d], recv_sem=rsem.at[d],
                device_id=peers[d], device_id_type=MESH,
            )
            for d in range(size - 1)
        ]
        for c in copies:
            c.start()
        between()
        for c in copies:
            c.wait()
        got = [inbox[d] for d in range(size - 1)]
        means = [mean] + [g[0:1] for g in got]
        whole = sum(means) * (1.0 / size)
        squares = square + sum(g[1:2] for g in got)
        for m in means:
            squares = squares + count * ((m - whole) * (m - whole))
        return whole, squares

    def frames_away():
        @pl.when(sends_on)
        def _():
            back(0).start()
            for i in range(len(PIECES)):
                bulk(i).start()

    def edges_away():
        @pl.when(up_on)
        def _():
            own_edge(0).start()

        @pl.when(down_on)
        def _():
            own_edge(1).start()

    pl.semaphore_wait(barrier, len(tm_peers) + len(row_peers))
    mean, square = exchange(
        mean, square, pixels, tm_peers, tm_out, tm_in, tm_send, tm_recv, frames_away
    )
    mean, square = exchange(
        mean, square, pixels * n_tm, row_peers, row_out, row_in, row_send, row_recv, edges_away
    )
    channel_mean = mean
    mean = over_group(channel_mean) * (1.0 / per_group)
    off = channel_mean - mean
    square = over_group(square + (pixels * n_tm * n_rows) * (off * off))
    inverse = lax.rsqrt(square * (1.0 / cells) + EPS)
    vector.wait()
    scale = 0.5 * (inverse * gv[pl.ds(0, ch)].reshape(1, ch))
    shift = 0.5 * gv[pl.ds(ch, ch)].reshape(1, ch)

    def normalize(src, f, dst, row):
        h = (src[f, row].astype(F32) - mean) * scale + shift
        h = h + h * jnp.tanh(h)
        if row == 0:
            h = jnp.where(up_on, h, 0.0)
        if row == height + 1:
            h = jnp.where(down_on, h, 0.0)
        dst[row] = h.astype(BF16)

    def norms(src, f, dst, rows):
        return [functools.partial(normalize, src, f, dst, row) for row in rows]

    cut = 4 * 256

    def lhs_of(used, first, rows):
        return jnp.concatenate(
            [
                act[pl.ds(first + kh, rows)].reshape(rows * width, ch)
                for act in used
                for kh in range(3)
            ],
            axis=1,
        )

    def put(t, first, rows, lo, got, add):
        got = got.reshape(rows, width, got.shape[1])
        at = (t, pl.ds(first, rows), slice(None), pl.ds(lo, got.shape[2]))
        z[at] = z[at] + got if add else got

    def weights(kt, n, lo, size):
        return wv[pl.ds(kt, n), :, :, pl.ds(lo, size)].reshape(n * 3 * ch, size)

    def main(t, used, kt, first, rows, add):
        def tile(lo):
            got = jnp.dot(
                lhs_of(used, first, rows), weights(kt, len(used), lo, 256), preferred_element_type=F32
            )
            put(t, first, rows, lo, got, add)

        return [functools.partial(tile, lo) for lo in range(0, cut, 256)]

    def pair(act, kts, first, rows, add):
        def tile():
            rhs = jnp.concatenate([weights(kt, 1, cut, 128) for kt in kts], axis=1)
            got = jnp.dot(lhs_of((act,), first, rows), rhs, preferred_element_type=F32)
            put(0, first, rows, cut, got[:, :128], add)
            put(1, first, rows, cut, got[:, 128:], add)

        return [tile]

    def single(t, act, kt, first, rows):
        def tile():
            got = jnp.dot(
                lhs_of((act,), first, rows), weights(kt, 1, cut, 128), preferred_element_type=F32
            )
            put(t, first, rows, cut, got, True)

        return [tile]

    def run(tiles, side=()):
        done = 0
        for i, tile in enumerate(tiles):
            tile()
            upto = len(side) * (i + 1) // len(tiles)
            for task in side[done:upto]:
                task()
            done = upto

    wi = lax.broadcasted_iota(jnp.int32, (width, ch), 0)

    def finish(t, h):
        left = pltpu.roll(z[t, h, :, 0:ch], 1, 0)
        right = pltpu.roll(z[t, h, :, 2 * ch : 3 * ch], width - 1, 0)
        conv = z[t, h, :, ch : 2 * ch]
        conv = conv + jnp.where(wi == 0, 0.0, left) + jnp.where(wi == width - 1, 0.0, right)
        cbias = gv[pl.ds(2 * ch, ch)].reshape(1, ch)
        out[0, t, h] = (xo[t, h + 1].astype(F32) + conv + cbias).astype(BF16)

    def finishes(t, first, rows):
        return [functools.partial(finish, t, h) for h in range(first, first + rows)]

    def forward(f):
        @pl.when(recvs_on)
        def _():
            a, b = [i for i, p in enumerate(PIECES) if p[0] == f][:2]
            bulk(a).wait_recv()
            bulk(b).wait_recv()

            @pl.when(up_on)
            def _():
                fwd_edge(f, 0).start()

            @pl.when(down_on)
            def _():
                fwd_edge(f, 1).start()

    def edge_in(f, i):
        @pl.when(down_on if i == 0 else up_on)
        def _():
            fwd_edge(f, i).wait_recv()

    @pl.when(down_on)
    def _():
        own_edge(0).wait_recv()

    @pl.when(up_on)
    def _():
        own_edge(1).wait_recv()

    low, high = range(0, half + 2), range(half + 2, height + 2)
    for task in norms(xo, 0, act_c, low):
        task()
    for c in wloads:
        c.wait()

    def own(first, side0, side1):
        run(
            main(0, (act_c,), 2, first, half, False) + pair(act_c, (2, 1), first, half, False), side0
        )
        forwards[first]()
        run(
            main(1, (act_c, act_d), 1, first, half, False) + single(1, act_d, 2, first, half), side1
        )

    def after_first():
        @pl.when(second_on)
        def _():
            back(0).wait_recv()
            back(1).start()

        forward(1)

    def before_last():
        @pl.when(recvs_on)
        def _():
            edge_in(1, 1)
            bulk(2).wait_recv()

    forwards = {0: after_first, half: before_last}
    own(0, norms(xo, 1, act_d, low), norms(xo, 0, act_c, high) + norms(xo, 1, act_d, high))
    own(half, (), norms(xr, 1, act_b, low))

    @pl.when(third_on)
    def _():
        back(1).wait_recv()
        back(2).start()

    @pl.when(recvs_on)
    def _():
        run(main(0, (act_b,), 1, 0, half, True))
        edge_in(1, 0)
        bulk(3).wait_recv()
        run(
            main(1, (act_b,), 0, 0, half, True) + pair(act_b, (1, 0), 0, half, True),
            norms(xr, 1, act_b, high),
        )
        run(
            main(0, (act_b,), 1, half, half, True)
            + main(1, (act_b,), 0, half, half, True)
            + pair(act_b, (1, 0), half, half, True),
            finishes(1, 0, half),
        )

    forward(0)

    @pl.when(recvs_on)
    def _():
        for task in finishes(1, half, half):
            task()
        bulk(6).wait_recv()
        for task in norms(xr, 0, act_a, (1, 2, 3, 8)):
            task()
        edge_in(0, 0)
        edge_in(0, 1)
        for task in norms(xr, 0, act_a, (0, 9)):
            task()
        back(2).wait_recv()
        for task in norms(xr, 0, act_a, (4, 5, 6)):
            task()
        run(main(0, (act_a,), 0, 0, half, True) + single(0, act_a, 0, 0, half))
        bulk(7).wait_recv()
        for task in norms(xr, 0, act_a, (7,)):
            task()
        run(
            main(0, (act_a,), 0, half, half, True) + single(0, act_a, 0, half, half),
            finishes(0, 0, half),
        )
        for task in finishes(0, half, half):
            task()

    @pl.when(jnp.logical_not(recvs_on))
    def _():
        for t in range(frames):
            for task in finishes(t, 0, height):
                task()

    @pl.when(sends_on)
    def _():
        for i in range(len(PIECES)):
            bulk(i).wait_send()
        back(0).wait_send()

    @pl.when(second_on)
    def _():
        back(1).wait_send()

    @pl.when(third_on)
    def _():
        back(2).wait_send()

    for i, on in ((0, up_on), (1, down_on)):

        @pl.when(on)
        def _():
            own_edge(i).wait_send()

            @pl.when(recvs_on)
            def _():
                for f in range(2):
                    fwd_edge(f, i).wait_send()


def shards(inputs, norm_gain, norm_bias, conv_weight, conv_bias):
    clips, frames, height, width, ch = inputs.shape
    n_tm, n_rows = lax.axis_size("tm"), lax.axis_size("rows")
    per_group = ch // GROUPS
    cells = 1.0 * clips * frames * height * width * per_group * n_tm * n_rows
    hbm = pl.BlockSpec(memory_space=pltpu.HBM)
    dma = lambda n: pltpu.SemaphoreType.DMA((n,))
    act = pltpu.VMEM((height + 2, width, ch), BF16)
    hop = pltpu.VMEM((BACK[1], width, ch), BF16)
    return pl.pallas_call(
        functools.partial(kernel, cells, per_group),
        out_shape=jax.ShapeDtypeStruct(inputs.shape, BF16),
        in_specs=[hbm] * 3,
        out_specs=pl.BlockSpec(memory_space=pltpu.VMEM),
        scratch_shapes=[
            pltpu.VMEM((frames, height + 2, width, ch), BF16),
            pltpu.VMEM((2, height + 2, width, ch), BF16),
            act,
            act,
            act,
            act,
            pltpu.VMEM((3, 3, ch, 3 * ch), BF16),
            pltpu.VMEM((frames, height, width, 3 * ch), F32),
            pltpu.VMEM((ch, ch), BF16),
            pltpu.VMEM((2, ch), F32),
            pltpu.VMEM((n_tm - 1, 2, ch), F32),
            pltpu.VMEM((2, ch), F32),
            pltpu.VMEM((n_rows - 1, 2, ch), F32),
            hop,
            hop,
            pltpu.VMEM((3 * ch,), F32),
            pltpu.SemaphoreType.DMA,
            dma(3),
            pltpu.SemaphoreType.DMA,
            dma(len(PIECES)),
            dma(len(PIECES)),
            dma(3),
            dma(3),
            dma(2),
            dma(2),
            dma(4),
            dma(4),
            dma(n_tm - 1),
            dma(n_tm - 1),
            dma(n_rows - 1),
            dma(n_rows - 1),
        ],
        compiler_params=pltpu.CompilerParams(
            collective_id=0, has_side_effects=True, vmem_limit_bytes=51 * 1024 * 1024
        ),
    )(inputs, jnp.concatenate([norm_gain, norm_bias, conv_bias]), conv_weight)


def solution(mesh):
    placed = (P("batch", "tm", "rows", None, None), P(), P(), P(), P())
    return jax.shard_map(
        shards,
        mesh=mesh,
        in_specs=placed,
        out_specs=P("batch", "tm", "rows", None, None),
        check_vma=False,
    )
```

```python
import functools

import jax
import jax.numpy as jnp
from jax import lax
from jax.experimental import pallas as pl
from jax.experimental.pallas import tpu as pltpu
from jax.sharding import PartitionSpec as P

MESH = pl.DeviceIdType.MESH
GROUPS = 32
EPS = 1e-06
F32 = jnp.float32
BF16 = jnp.bfloat16

PIECES = ((1, 0, 1), (1, 7, 1), (1, 1, 4), (1, 5, 2), (0, 0, 1), (0, 7, 1), (0, 3, 2))
BACK = ((1, 2), (5, 2))


def kernel(
    cells, per_group,
    x, vec, w, out,
    xo, xr, act_a, act_b, act_c, act_d, wv, z, ind, tm_out, tm_in, row_out, row_in, hop1, hop2, gv,
    load_sem, wsem, vec_sem,
    bulk_send, bulk_recv, back_send, back_recv, halo_send, halo_recv, fwd_send, fwd_recv,
    tm_send, tm_recv, row_send, row_recv,
):
    n_tm, n_rows = lax.axis_size("tm"), lax.axis_size("rows")
    j, r = lax.axis_index("tm"), lax.axis_index("rows")
    frames, height, width, ch = xo.shape[0], xo.shape[1] - 2, xo.shape[2], xo.shape[3]
    half = height // 2

    load = pltpu.make_async_copy(x.at[0], xo.at[:, 1 : height + 1], load_sem)
    load.start()
    vector = pltpu.make_async_copy(vec, gv, vec_sem)
    vector.start()
    wloads = [
        pltpu.make_async_copy(w.at[:, :, kw], wv.at[:, :, :, pl.ds(kw * ch, ch)], wsem.at[kw])
        for kw in range(3)
    ]
    for c in wloads:
        c.start()

    barrier = pltpu.get_barrier_semaphore()
    tm_peers = [{"tm": lax.rem(j + d, n_tm)} for d in range(1, n_tm)]
    row_peers = [{"rows": lax.rem(r + d, n_rows)} for d in range(1, n_rows)]
    for peer in tm_peers + row_peers:
        pl.semaphore_signal(barrier, inc=1, device_id=peer, device_id_type=MESH)

    def bulk(i):
        f, first, rows = PIECES[i]
        return pltpu.make_async_remote_copy(
            src_ref=xo.at[f, pl.ds(1 + first, rows)],
            dst_ref=xr.at[f, pl.ds(1 + first, rows)],
            send_sem=bulk_send.at[i],
            recv_sem=bulk_recv.at[i],
            device_id={"tm": lax.rem(j + 1, n_tm)},
            device_id_type=MESH,
        )

    def back(hop, p):
        first, rows = BACK[p]
        mine, place = xo.at[0, pl.ds(1 + first, rows)], xr.at[0, pl.ds(1 + first, rows)]
        line = (mine, hop1.at[p, pl.ds(0, rows)], hop2.at[p, pl.ds(0, rows)], place)
        return pltpu.make_async_remote_copy(
            src_ref=line[hop], dst_ref=line[hop + 1],
            send_sem=back_send.at[len(BACK) * hop + p], recv_sem=back_recv.at[len(BACK) * hop + p],
            device_id={"tm": lax.rem(j + n_tm - 1, n_tm)}, device_id_type=MESH,
        )

    def pass_back(hop, p):
        back(hop - 1, p).wait_recv()
        back(hop, p).start()

    def edge(i, src, dst, ssem, rsem):
        return pltpu.make_async_remote_copy(
            src_ref=src, dst_ref=dst, send_sem=ssem, recv_sem=rsem,
            device_id={"rows": lax.rem(r + (n_rows - 1 if i == 0 else 1), n_rows)},
            device_id_type=MESH,
        )

    def own_edge(i):
        return edge(
            i, xo.at[:, 1 if i == 0 else height], xo.at[:, height + 1 if i == 0 else 0],
            halo_send.at[i], halo_recv.at[i],
        )

    def fwd_edge(f, i):
        return edge(
            i, xr.at[f, 1 if i == 0 else height], xr.at[f, height + 1 if i == 0 else 0],
            fwd_send.at[2 * f + i], fwd_recv.at[2 * f + i],
        )

    recvs_on, up_on, down_on = j > 0, r > 0, r < n_rows - 1

    a = lax.broadcasted_iota(jnp.int32, (ch, ch), 0)
    b = lax.broadcasted_iota(jnp.int32, (ch, ch), 1)
    group_of = lambda i: lax.shift_right_logical(i * 43691, 19)
    ind[...] = jnp.where(group_of(a) == group_of(b), 1.0, 0.0).astype(BF16)

    def over_group(v):
        v = jnp.broadcast_to(v, (8, ch))
        hi = v.astype(BF16).astype(F32)
        mid = (v - hi).astype(BF16).astype(F32)
        lo = v - hi - mid
        parts = jnp.concatenate([hi, mid, lo, jnp.zeros_like(v)], axis=0).astype(BF16)
        got = jnp.dot(parts, ind[...], preferred_element_type=F32)
        return got[0:1] + (got[8:9] + got[16:17])

    load.wait()
    pixels = 1.0 * frames * height * width

    def fold(v):
        return jnp.sum(v.reshape(-1, 32, ch), axis=0)

    def over_rows(v):
        return jnp.sum(v, axis=0, keepdims=True)

    pivot = over_rows(fold(xo[0, 1].astype(F32))) * (1.0 / width)

    def sums(i, acc):
        first, second = acc
        d = xo[lax.div(i, height), 1 + lax.rem(i, height)].astype(F32) - pivot
        return first + fold(d), second + fold(d * d)

    zero = jnp.zeros((32, ch), F32)
    first, second = lax.fori_loop(0, frames * height, sums, (zero, zero))
    first, second = over_rows(first), over_rows(second)
    mean = pivot + first * (1.0 / pixels)
    square = second - first * (first * (1.0 / pixels))

    top = lax.broadcasted_iota(jnp.int32, (2, ch), 0) == 0

    def exchange(mean, square, count, peers, outbox, inbox, ssem, rsem, between):
        size = len(peers) + 1
        outbox[...] = jnp.where(top, mean, square)
        copies = [
            pltpu.make_async_remote_copy(
                src_ref=outbox, dst_ref=inbox.at[d], send_sem=ssem.at[d], recv_sem=rsem.at[d],
                device_id=peers[d], device_id_type=MESH,
            )
            for d in range(size - 1)
        ]
        for c in copies:
            c.start()
        between()
        for c in copies:
            c.wait()
        got = [inbox[d] for d in range(size - 1)]
        means = [mean] + [g[0:1] for g in got]
        whole = sum(means) * (1.0 / size)
        squares = square + sum(g[1:2] for g in got)
        for m in means:
            squares = squares + count * ((m - whole) * (m - whole))
        return whole, squares

    def frames_away():
        for p in range(len(BACK)):
            back(0, p).start()
        for i in range(len(PIECES)):
            bulk(i).start()
        own_edge(0).start()
        own_edge(1).start()

    pl.semaphore_wait(barrier, len(tm_peers) + len(row_peers))
    mean, square = exchange(
        mean, square, pixels, tm_peers, tm_out, tm_in, tm_send, tm_recv, frames_away
    )
    mean, square = exchange(
        mean, square, pixels * n_tm, row_peers, row_out, row_in, row_send, row_recv, lambda: None
    )
    pass_back(1, 0)
    channel_mean = mean
    mean = over_group(channel_mean) * (1.0 / per_group)
    off = channel_mean - mean
    square = over_group(square + (pixels * n_tm * n_rows) * (off * off))
    inverse = lax.rsqrt(square * (1.0 / cells) + EPS)
    vector.wait()
    scale = 0.5 * (inverse * gv[pl.ds(0, ch)].reshape(1, ch))
    shift = 0.5 * gv[pl.ds(ch, ch)].reshape(1, ch)

    def kept(on):
        return jnp.where(on, scale, 0.0), jnp.where(on, shift, 0.0)

    factors = [kept(up_on), (scale, shift), kept(down_on)]

    def normalize(src, f, dst, row):
        by, plus = factors[0 if row == 0 else 2 if row == height + 1 else 1]
        h = (src[f, row].astype(F32) - mean) * by + plus
        dst[row] = (h + h * jnp.tanh(h)).astype(BF16)

    def norms(src, f, dst, rows):
        return [functools.partial(normalize, src, f, dst, row) for row in rows]

    cut = 4 * 256

    def lhs_of(used, first, rows):
        return jnp.concatenate(
            [
                act[pl.ds(first + kh, rows)].reshape(rows * width, ch)
                for act in used
                for kh in range(3)
            ],
            axis=1,
        )

    def put(t, first, rows, lo, got, add):
        got = got.reshape(rows, width, got.shape[1])
        at = (t, pl.ds(first, rows), slice(None), pl.ds(lo, got.shape[2]))
        z[at] = z[at] + got if add else got

    def weights(kt, n, lo, size):
        return wv[pl.ds(kt, n), :, :, pl.ds(lo, size)].reshape(n * 3 * ch, size)

    def main(t, used, kt, first, rows, add):
        def tile(lo):
            got = jnp.dot(
                lhs_of(used, first, rows), weights(kt, len(used), lo, 256), preferred_element_type=F32
            )
            put(t, first, rows, lo, got, add)

        return [functools.partial(tile, lo) for lo in range(0, cut, 256)]

    def pair(act, kts, first, rows, add):
        def tile():
            rhs = jnp.concatenate([weights(kt, 1, cut, 128) for kt in kts], axis=1)
            got = jnp.dot(lhs_of((act,), first, rows), rhs, preferred_element_type=F32)
            put(0, first, rows, cut, got[:, :128], add)
            put(1, first, rows, cut, got[:, 128:], add)

        return [tile]

    def single(t, act, kt, first, rows):
        def tile():
            got = jnp.dot(
                lhs_of((act,), first, rows), weights(kt, 1, cut, 128), preferred_element_type=F32
            )
            put(t, first, rows, cut, got, True)

        return [tile]

    def run(tiles, side=()):
        done = 0
        for i, tile in enumerate(tiles):
            tile()
            upto = len(side) * (i + 1) // len(tiles)
            for task in side[done:upto]:
                task()
            done = upto

    wi = lax.broadcasted_iota(jnp.int32, (width, ch), 0)

    def finish(t, h):
        left = pltpu.roll(z[t, h, :, 0:ch], 1, 0)
        right = pltpu.roll(z[t, h, :, 2 * ch : 3 * ch], width - 1, 0)
        conv = z[t, h, :, ch : 2 * ch]
        conv = conv + jnp.where(wi == 0, 0.0, left) + jnp.where(wi == width - 1, 0.0, right)
        cbias = gv[pl.ds(2 * ch, ch)].reshape(1, ch)
        out[0, t, h] = (xo[t, h + 1].astype(F32) + conv + cbias).astype(BF16)

    def finishes(t, first, rows):
        return [functools.partial(finish, t, h) for h in range(first, first + rows)]

    def forward(f):
        for i, p in enumerate(PIECES):
            if p in ((f, 0, 1), (f, height - 1, 1)):
                bulk(i).wait_recv()
        fwd_edge(f, 0).start()
        fwd_edge(f, 1).start()

    def edges_in(f):
        fwd_edge(f, 0).wait_recv()
        fwd_edge(f, 1).wait_recv()

    low, high = range(0, half + 2), range(half + 2, height + 2)
    forward(1)
    own_edge(0).wait_recv()
    own_edge(1).wait_recv()

    run(norms(xo, 0, act_c, low))
    for c in wloads:
        c.wait()
    run(
        main(0, (act_c,), 2, 0, half, False) + pair(act_c, (2, 1), 0, half, False),
        norms(xo, 1, act_d, low),
    )
    run(
        main(1, (act_c, act_d), 1, 0, half, False) + single(1, act_d, 2, 0, half),
        norms(xo, 0, act_c, high) + norms(xo, 1, act_d, high),
    )
    pass_back(1, 1)
    run(main(0, (act_c,), 2, half, half, False) + pair(act_c, (2, 1), half, half, False))
    pass_back(2, 0)
    edges_in(1)
    bulk(2).wait_recv()
    run(
        main(1, (act_c, act_d), 1, half, half, False) + single(1, act_d, 2, half, half),
        norms(xr, 1, act_b, low),
    )
    pass_back(2, 1)
    bulk(3).wait_recv()

    @pl.when(recvs_on)
    def _():
        run(
            main(0, (act_b,), 1, 0, half, True)
            + main(1, (act_b,), 0, 0, half, True)
            + pair(act_b, (1, 0), 0, half, True),
            norms(xr, 1, act_b, high),
        )
        forward(0)
        back(2, 0).wait_recv()
        run(
            main(0, (act_b,), 1, half, half, True)
            + main(1, (act_b,), 0, half, half, True)
            + pair(act_b, (1, 0), half, half, True),
            norms(xr, 0, act_a, (1, 2, 3, 8)) + finishes(1, 0, half),
        )
        bulk(6).wait_recv()
        back(2, 1).wait_recv()
        edges_in(0)
        run(norms(xr, 0, act_a, (0, 4, 5)))
        run(
            main(0, (act_a,), 0, 0, half, True) + single(0, act_a, 0, 0, half),
            norms(xr, 0, act_a, (6, 7, 9)) + finishes(1, half, half),
        )
        run(
            main(0, (act_a,), 0, half, 2, True) + single(0, act_a, 0, half, 2), finishes(0, 0, half)
        )
        run(
            main(0, (act_a,), 0, half + 2, 2, True) + single(0, act_a, 0, half + 2, 2),
            finishes(0, half, 2),
        )
        run(finishes(0, half + 2, 2))

    @pl.when(jnp.logical_not(recvs_on))
    def _():
        for t in range(frames):
            run(finishes(t, 0, height))
        forward(0)
        edges_in(0)
        bulk(6).wait_recv()
        for p in range(len(BACK)):
            back(2, p).wait_recv()

    for i in range(len(PIECES)):
        bulk(i).wait_send()
    for hop in range(3):
        for p in range(len(BACK)):
            back(hop, p).wait_send()
    for i in range(2):
        own_edge(i).wait_send()
        for f in range(2):
            fwd_edge(f, i).wait_send()


def shards(inputs, norm_gain, norm_bias, conv_weight, conv_bias):
    clips, frames, height, width, ch = inputs.shape
    n_tm, n_rows = lax.axis_size("tm"), lax.axis_size("rows")
    per_group = ch // GROUPS
    cells = 1.0 * clips * frames * height * width * per_group * n_tm * n_rows
    hbm = pl.BlockSpec(memory_space=pltpu.HBM)
    dma = lambda n: pltpu.SemaphoreType.DMA((n,))
    act = pltpu.VMEM((height + 2, width, ch), BF16)
    hop = pltpu.VMEM((len(BACK), BACK[0][1], width, ch), BF16)
    return pl.pallas_call(
        functools.partial(kernel, cells, per_group),
        out_shape=jax.ShapeDtypeStruct(inputs.shape, BF16),
        in_specs=[hbm] * 3,
        out_specs=pl.BlockSpec(memory_space=pltpu.VMEM),
        scratch_shapes=[
            pltpu.VMEM((frames, height + 2, width, ch), BF16),
            pltpu.VMEM((2, height + 2, width, ch), BF16),
            act,
            act,
            act,
            act,
            pltpu.VMEM((3, 3, ch, 3 * ch), BF16),
            pltpu.VMEM((frames, height, width, 3 * ch), F32),
            pltpu.VMEM((ch, ch), BF16),
            pltpu.VMEM((2, ch), F32),
            pltpu.VMEM((n_tm - 1, 2, ch), F32),
            pltpu.VMEM((2, ch), F32),
            pltpu.VMEM((n_rows - 1, 2, ch), F32),
            hop,
            hop,
            pltpu.VMEM((3 * ch,), F32),
            pltpu.SemaphoreType.DMA,
            dma(3),
            pltpu.SemaphoreType.DMA,
            dma(len(PIECES)),
            dma(len(PIECES)),
            dma(3 * len(BACK)),
            dma(3 * len(BACK)),
            dma(2),
            dma(2),
            dma(4),
            dma(4),
            dma(n_tm - 1),
            dma(n_tm - 1),
            dma(n_rows - 1),
            dma(n_rows - 1),
        ],
        compiler_params=pltpu.CompilerParams(
            collective_id=0, has_side_effects=True, vmem_limit_bytes=51 * 1024 * 1024
        ),
    )(inputs, jnp.concatenate([norm_gain, norm_bias, conv_bias]), conv_weight)


def solution(mesh):
    placed = (P("batch", "tm", "rows", None, None), P(), P(), P(), P())
    return jax.shard_map(
        shards,
        mesh=mesh,
        in_specs=placed,
        out_specs=P("batch", "tm", "rows", None, None),
        check_vma=False,
    )
```

```python
import functools

import jax
import jax.numpy as jnp
from jax import lax
from jax.experimental import pallas as pl
from jax.experimental.pallas import tpu as pltpu
from jax.sharding import PartitionSpec as P

MESH = pl.DeviceIdType.MESH
GROUPS = 32
EPS = 1e-06
F32 = jnp.float32
BF16 = jnp.bfloat16

PIECES = ((1, 0, 1), (1, 7, 1), (1, 1, 4), (1, 5, 2), (0, 0, 1), (0, 7, 1), (0, 3, 1), (0, 4, 1))
BACK = ((1, 2), (5, 2))


def kernel(
    cells, per_group,
    x, vec, w, out,
    xo, xr, act_a, act_b, act_c, act_d, wv, z, ind, tm_out, tm_in, row_out, row_in, hop1, hop2, gv,
    load_sem, wsem, vec_sem,
    bulk_send, bulk_recv, back_send, back_recv, halo_send, halo_recv, fwd_send, fwd_recv,
    tm_send, tm_recv, row_send, row_recv,
):
    n_tm, n_rows = lax.axis_size("tm"), lax.axis_size("rows")
    j, r = lax.axis_index("tm"), lax.axis_index("rows")
    frames, height, width, ch = xo.shape[0], xo.shape[1] - 2, xo.shape[2], xo.shape[3]
    half = height // 2

    load = pltpu.make_async_copy(x.at[0], xo.at[:, 1 : height + 1], load_sem)
    load.start()
    vector = pltpu.make_async_copy(vec, gv, vec_sem)
    vector.start()
    wloads = [
        pltpu.make_async_copy(w.at[:, :, kw], wv.at[:, :, :, pl.ds(kw * ch, ch)], wsem.at[kw])
        for kw in range(3)
    ]
    for c in wloads:
        c.start()

    barrier = pltpu.get_barrier_semaphore()
    tm_peers = [{"tm": lax.rem(j + d, n_tm)} for d in range(1, n_tm)]
    row_peers = [{"rows": lax.rem(r + d, n_rows)} for d in range(1, n_rows)]
    for peer in tm_peers + row_peers:
        pl.semaphore_signal(barrier, inc=1, device_id=peer, device_id_type=MESH)

    def bulk(i):
        f, first, rows = PIECES[i]
        return pltpu.make_async_remote_copy(
            src_ref=xo.at[f, pl.ds(1 + first, rows)],
            dst_ref=xr.at[f, pl.ds(1 + first, rows)],
            send_sem=bulk_send.at[i],
            recv_sem=bulk_recv.at[i],
            device_id={"tm": lax.rem(j + 1, n_tm)},
            device_id_type=MESH,
        )

    def back(hop, p):
        first, rows = BACK[p]
        mine, place = xo.at[0, pl.ds(1 + first, rows)], xr.at[0, pl.ds(1 + first, rows)]
        line = (mine, hop1.at[p, pl.ds(0, rows)], hop2.at[p, pl.ds(0, rows)], place)
        return pltpu.make_async_remote_copy(
            src_ref=line[hop], dst_ref=line[hop + 1],
            send_sem=back_send.at[len(BACK) * hop + p], recv_sem=back_recv.at[len(BACK) * hop + p],
            device_id={"tm": lax.rem(j + n_tm - 1, n_tm)}, device_id_type=MESH,
        )

    def pass_back(hop, p):
        back(hop - 1, p).wait_recv()
        back(hop, p).start()

    def edge(i, src, dst, ssem, rsem):
        return pltpu.make_async_remote_copy(
            src_ref=src, dst_ref=dst, send_sem=ssem, recv_sem=rsem,
            device_id={"rows": lax.rem(r + (n_rows - 1 if i == 0 else 1), n_rows)},
            device_id_type=MESH,
        )

    def own_edge(i):
        return edge(
            i, xo.at[:, 1 if i == 0 else height], xo.at[:, height + 1 if i == 0 else 0],
            halo_send.at[i], halo_recv.at[i],
        )

    def fwd_edge(f, i):
        return edge(
            i, xr.at[f, 1 if i == 0 else height], xr.at[f, height + 1 if i == 0 else 0],
            fwd_send.at[2 * f + i], fwd_recv.at[2 * f + i],
        )

    recvs_on, up_on, down_on = j > 0, r > 0, r < n_rows - 1

    a = lax.broadcasted_iota(jnp.int32, (ch, ch), 0)
    b = lax.broadcasted_iota(jnp.int32, (ch, ch), 1)
    group_of = lambda i: lax.shift_right_logical(i * 43691, 19)
    ind[...] = jnp.where(group_of(a) == group_of(b), 1.0, 0.0).astype(BF16)

    def over_group(v):
        v = jnp.broadcast_to(v, (8, ch))
        hi = v.astype(BF16).astype(F32)
        mid = (v - hi).astype(BF16).astype(F32)
        lo = v - hi - mid
        parts = jnp.concatenate([hi, mid, lo, jnp.zeros_like(v)], axis=0).astype(BF16)
        got = jnp.dot(parts, ind[...], preferred_element_type=F32)
        return got[0:1] + (got[8:9] + got[16:17])

    load.wait()
    pixels = 1.0 * frames * height * width

    def fold(v):
        return jnp.sum(v.reshape(-1, 32, ch), axis=0)

    def over_rows(v):
        return jnp.sum(v, axis=0, keepdims=True)

    pivot = over_rows(fold(xo[0, 1].astype(F32))) * (1.0 / width)

    def sums(i, acc):
        first, second = acc
        d = xo[lax.div(i, height), 1 + lax.rem(i, height)].astype(F32) - pivot
        return first + fold(d), second + fold(d * d)

    zero = jnp.zeros((32, ch), F32)
    first, second = lax.fori_loop(0, frames * height, sums, (zero, zero))
    first, second = over_rows(first), over_rows(second)
    mean = pivot + first * (1.0 / pixels)
    square = second - first * (first * (1.0 / pixels))

    top = lax.broadcasted_iota(jnp.int32, (2, ch), 0) == 0

    def exchange(mean, square, count, peers, outbox, inbox, ssem, rsem, between):
        size = len(peers) + 1
        outbox[...] = jnp.where(top, mean, square)
        copies = [
            pltpu.make_async_remote_copy(
                src_ref=outbox, dst_ref=inbox.at[d], send_sem=ssem.at[d], recv_sem=rsem.at[d],
                device_id=peers[d], device_id_type=MESH,
            )
            for d in range(size - 1)
        ]
        for c in copies:
            c.start()
        between()
        for c in copies:
            c.wait()
        got = [inbox[d] for d in range(size - 1)]
        means = [mean] + [g[0:1] for g in got]
        whole = sum(means) * (1.0 / size)
        squares = square + sum(g[1:2] for g in got)
        for m in means:
            squares = squares + count * ((m - whole) * (m - whole))
        return whole, squares

    def frames_away():
        for p in range(len(BACK)):
            back(0, p).start()
        for i in range(len(PIECES)):
            bulk(i).start()
        own_edge(0).start()
        own_edge(1).start()

    pl.semaphore_wait(barrier, len(tm_peers) + len(row_peers))
    mean, square = exchange(
        mean, square, pixels, tm_peers, tm_out, tm_in, tm_send, tm_recv, frames_away
    )
    mean, square = exchange(
        mean, square, pixels * n_tm, row_peers, row_out, row_in, row_send, row_recv, lambda: None
    )
    pass_back(1, 0)
    channel_mean = mean
    mean = over_group(channel_mean) * (1.0 / per_group)
    off = channel_mean - mean
    square = over_group(square + (pixels * n_tm * n_rows) * (off * off))
    inverse = lax.rsqrt(square * (1.0 / cells) + EPS)
    vector.wait()
    scale = 0.5 * (inverse * gv[pl.ds(0, ch)].reshape(1, ch))
    shift = 0.5 * gv[pl.ds(ch, ch)].reshape(1, ch)

    def kept(on):
        return jnp.where(on, scale, 0.0), jnp.where(on, shift, 0.0)

    factors = [kept(up_on), (scale, shift), kept(down_on)]

    def normalize(src, f, dst, row):
        by, plus = factors[0 if row == 0 else 2 if row == height + 1 else 1]
        h = (src[f, row].astype(F32) - mean) * by + plus
        dst[row] = (h + h * jnp.tanh(h)).astype(BF16)

    def norms(src, f, dst, rows):
        return [functools.partial(normalize, src, f, dst, row) for row in rows]

    cut = 4 * 256

    def lhs_of(used, first, rows):
        return jnp.concatenate(
            [
                act[pl.ds(first + kh, rows)].reshape(rows * width, ch)
                for act in used
                for kh in range(3)
            ],
            axis=1,
        )

    def put(t, first, rows, lo, got, add):
        got = got.reshape(rows, width, got.shape[1])
        at = (t, pl.ds(first, rows), slice(None), pl.ds(lo, got.shape[2]))
        z[at] = z[at] + got if add else got

    def weights(kt, n, lo, size):
        return wv[pl.ds(kt, n), :, :, pl.ds(lo, size)].reshape(n * 3 * ch, size)

    def main(t, used, kt, first, rows, add):
        def tile(lo):
            got = jnp.dot(
                lhs_of(used, first, rows), weights(kt, len(used), lo, 256), preferred_element_type=F32
            )
            put(t, first, rows, lo, got, add)

        return [functools.partial(tile, lo) for lo in range(0, cut, 256)]

    def pair(act, kts, first, rows, add):
        def tile():
            rhs = jnp.concatenate([weights(kt, 1, cut, 128) for kt in kts], axis=1)
            got = jnp.dot(lhs_of((act,), first, rows), rhs, preferred_element_type=F32)
            put(0, first, rows, cut, got[:, :128], add)
            put(1, first, rows, cut, got[:, 128:], add)

        return [tile]

    def single(t, act, kt, first, rows):
        def tile():
            got = jnp.dot(
                lhs_of((act,), first, rows), weights(kt, 1, cut, 128), preferred_element_type=F32
            )
            put(t, first, rows, cut, got, True)

        return [tile]

    def some(first, rows, khs):
        def tile(lo):
            n = min(256, 3 * ch - lo)
            lhs = jnp.concatenate(
                [act_a[pl.ds(first + kh, rows)].reshape(rows * width, ch) for kh in khs], axis=1
            )
            rhs = jnp.concatenate([wv[0, kh, :, pl.ds(lo, n)] for kh in khs], axis=0)
            put(0, first, rows, lo, jnp.dot(lhs, rhs, preferred_element_type=F32), True)

        return [functools.partial(tile, lo) for lo in range(0, 3 * ch, 256)]

    def run(tiles, side=()):
        done = 0
        for i, tile in enumerate(tiles):
            tile()
            upto = len(side) * (i + 1) // len(tiles)
            for task in side[done:upto]:
                task()
            done = upto

    wi = lax.broadcasted_iota(jnp.int32, (width, ch), 0)

    def finish(t, h):
        left = pltpu.roll(z[t, h, :, 0:ch], 1, 0)
        right = pltpu.roll(z[t, h, :, 2 * ch : 3 * ch], width - 1, 0)
        conv = z[t, h, :, ch : 2 * ch]
        conv = conv + jnp.where(wi == 0, 0.0, left) + jnp.where(wi == width - 1, 0.0, right)
        cbias = gv[pl.ds(2 * ch, ch)].reshape(1, ch)
        out[0, t, h] = (xo[t, h + 1].astype(F32) + conv + cbias).astype(BF16)

    def finishes(t, first, rows):
        return [functools.partial(finish, t, h) for h in range(first, first + rows)]

    def forward(f):
        for i, p in enumerate(PIECES):
            if p in ((f, 0, 1), (f, height - 1, 1)):
                bulk(i).wait_recv()
        fwd_edge(f, 0).start()
        fwd_edge(f, 1).start()

    def edges_in(f):
        fwd_edge(f, 0).wait_recv()
        fwd_edge(f, 1).wait_recv()

    low, high = range(0, half + 2), range(half + 2, height + 2)
    forward(1)
    own_edge(0).wait_recv()
    own_edge(1).wait_recv()

    run(norms(xo, 0, act_c, low))
    for c in wloads:
        c.wait()
    run(
        main(0, (act_c,), 2, 0, half, False) + pair(act_c, (2, 1), 0, half, False),
        norms(xo, 1, act_d, low),
    )
    run(
        main(1, (act_c, act_d), 1, 0, half, False) + single(1, act_d, 2, 0, half),
        norms(xo, 0, act_c, high) + norms(xo, 1, act_d, high),
    )
    pass_back(1, 1)
    edges_in(1)
    run(
        pair(act_c, (2, 1), half, half, False)
        + main(1, (act_c, act_d), 1, half, half, False)
        + single(1, act_d, 2, half, half),
        norms(xr, 1, act_b, (0, 1, 8, 9)),
    )
    pass_back(2, 0)

    @pl.when(recvs_on)
    def _():
        bulk(2).wait_recv()
        run(norms(xr, 1, act_b, (2, 3, 4, 5)))
        run(
            main(0, (act_b,), 1, 0, half, True)
            + main(1, (act_b,), 0, 0, half, True)
            + pair(act_b, (1, 0), 0, half, True)
        )
        pass_back(2, 1)
        bulk(3).wait_recv()
        run(norms(xr, 1, act_b, (6, 7)))
        run(
            main(0, (act_b, act_c), 1, half, half, False) + main(1, (act_b,), 0, half, half, True),
            finishes(1, 0, half),
        )
        forward(0)
        back(2, 0).wait_recv()
        run(pair(act_b, (1, 0), half, half, True), norms(xr, 0, act_a, (1, 2, 3)))
        run(
            some(1, 1, (0, 1, 2)) + some(0, 1, (1, 2)) + some(2, 1, (0, 1)) + some(3, 1, (0,)),
            norms(xr, 0, act_a, (8,)) + finishes(1, half, half),
        )
        bulk(6).wait_recv()
        run(norms(xr, 0, act_a, (4,)))
        run(
            some(3, 1, (1,)) + some(2, 1, (2,)) + some(4, 1, (0,)) + some(6, 1, (2,)) + some(7, 1, (1,)),
            finishes(0, 1, 2),
        )
        bulk(7).wait_recv()
        back(2, 1).wait_recv()
        edges_in(0)
        run(norms(xr, 0, act_a, (5, 0)))
        run(some(3, 1, (2,)) + some(0, 1, (0,)), norms(xr, 0, act_a, (6, 7, 9)))
        run(some(4, 1, (1, 2)), finishes(0, 0, 1))
        run(some(5, 1, (0, 1, 2)), finishes(0, 3, 2))
        run(some(6, 1, (0, 1)), finishes(0, 5, 1))
        run(some(7, 1, (0, 2)), finishes(0, 6, 1))
        run(finishes(0, 7, 1))

    @pl.when(jnp.logical_not(recvs_on))
    def _():
        run(main(0, (act_c,), 2, half, half, False))
        pass_back(2, 1)
        for t in range(frames):
            run(finishes(t, 0, height))
        forward(0)
        edges_in(0)
        for i in (2, 3, 6, 7):
            bulk(i).wait_recv()
        for p in range(len(BACK)):
            back(2, p).wait_recv()

    for i in range(len(PIECES)):
        bulk(i).wait_send()
    for hop in range(3):
        for p in range(len(BACK)):
            back(hop, p).wait_send()
    for i in range(2):
        own_edge(i).wait_send()
        for f in range(2):
            fwd_edge(f, i).wait_send()


def shards(inputs, norm_gain, norm_bias, conv_weight, conv_bias):
    clips, frames, height, width, ch = inputs.shape
    n_tm, n_rows = lax.axis_size("tm"), lax.axis_size("rows")
    per_group = ch // GROUPS
    cells = 1.0 * clips * frames * height * width * per_group * n_tm * n_rows
    hbm = pl.BlockSpec(memory_space=pltpu.HBM)
    dma = lambda n: pltpu.SemaphoreType.DMA((n,))
    act = pltpu.VMEM((height + 2, width, ch), BF16)
    hop = pltpu.VMEM((len(BACK), BACK[0][1], width, ch), BF16)
    return pl.pallas_call(
        functools.partial(kernel, cells, per_group),
        out_shape=jax.ShapeDtypeStruct(inputs.shape, BF16),
        in_specs=[hbm] * 3,
        out_specs=pl.BlockSpec(memory_space=pltpu.VMEM),
        scratch_shapes=[
            pltpu.VMEM((frames, height + 2, width, ch), BF16),
            pltpu.VMEM((2, height + 2, width, ch), BF16),
            act,
            act,
            act,
            act,
            pltpu.VMEM((3, 3, ch, 3 * ch), BF16),
            pltpu.VMEM((frames, height, width, 3 * ch), F32),
            pltpu.VMEM((ch, ch), BF16),
            pltpu.VMEM((2, ch), F32),
            pltpu.VMEM((n_tm - 1, 2, ch), F32),
            pltpu.VMEM((2, ch), F32),
            pltpu.VMEM((n_rows - 1, 2, ch), F32),
            hop,
            hop,
            pltpu.VMEM((3 * ch,), F32),
            pltpu.SemaphoreType.DMA,
            dma(3),
            pltpu.SemaphoreType.DMA,
            dma(len(PIECES)),
            dma(len(PIECES)),
            dma(3 * len(BACK)),
            dma(3 * len(BACK)),
            dma(2),
            dma(2),
            dma(4),
            dma(4),
            dma(n_tm - 1),
            dma(n_tm - 1),
            dma(n_rows - 1),
            dma(n_rows - 1),
        ],
        compiler_params=pltpu.CompilerParams(
            collective_id=0, has_side_effects=True, vmem_limit_bytes=51 * 1024 * 1024
        ),
    )(inputs, jnp.concatenate([norm_gain, norm_bias, conv_bias]), conv_weight)


def solution(mesh):
    placed = (P("batch", "tm", "rows", None, None), P(), P(), P(), P())
    return jax.shard_map(
        shards,
        mesh=mesh,
        in_specs=placed,
        out_specs=P("batch", "tm", "rows", None, None),
        check_vma=False,
    )
```

```python
import functools

import jax
import jax.numpy as jnp
from jax import lax
from jax.experimental import pallas as pl
from jax.experimental.pallas import tpu as pltpu
from jax.sharding import PartitionSpec as P

MESH = pl.DeviceIdType.MESH
GROUPS = 32
EPS = 1e-06
F32 = jnp.float32
BF16 = jnp.bfloat16

PIECES = ((1, 0, 1), (1, 7, 1), (1, 1, 4), (1, 5, 2), (0, 0, 1), (0, 7, 1), (0, 3, 1), (0, 5, 1))
BACK = ((1, 2), (4, 1), (6, 1))


def kernel(
    cells, per_group,
    x, gain, bias, cbias, w, out,
    xo, xr, act_a, act_b, act_c, act_d, wv, z, ind, tm_out, tm_in, row_out, row_in, hop1, hop2, gv,
    load_sem, wsem, vec_sem,
    bulk_send, bulk_recv, back_send, back_recv, halo_send, halo_recv, fwd_send, fwd_recv,
    tm_send, tm_recv, row_send, row_recv,
):
    n_tm, n_rows = lax.axis_size("tm"), lax.axis_size("rows")
    j, r = lax.axis_index("tm"), lax.axis_index("rows")
    frames, height, width, ch = xo.shape[0], xo.shape[1] - 2, xo.shape[2], xo.shape[3]
    half = height // 2

    load = pltpu.make_async_copy(x.at[0], xo.at[:, 1 : height + 1], load_sem)
    load.start()
    vectors = [
        pltpu.make_async_copy(v, gv.at[pl.ds(i * ch, ch)], vec_sem.at[i])
        for i, v in enumerate((gain, bias, cbias))
    ]
    for c in vectors:
        c.start()
    wloads = [
        pltpu.make_async_copy(w.at[:, :, kw], wv.at[:, :, :, pl.ds(kw * ch, ch)], wsem.at[kw])
        for kw in range(3)
    ]
    for c in wloads:
        c.start()

    barrier = pltpu.get_barrier_semaphore()
    tm_peers = [{"tm": lax.rem(j + d, n_tm)} for d in range(1, n_tm)]
    row_peers = [{"rows": lax.rem(r + d, n_rows)} for d in range(1, n_rows)]
    for peer in tm_peers + row_peers:
        pl.semaphore_signal(barrier, inc=1, device_id=peer, device_id_type=MESH)

    def bulk(i):
        f, first, rows = PIECES[i]
        return pltpu.make_async_remote_copy(
            src_ref=xo.at[f, pl.ds(1 + first, rows)],
            dst_ref=xr.at[f, pl.ds(1 + first, rows)],
            send_sem=bulk_send.at[i],
            recv_sem=bulk_recv.at[i],
            device_id={"tm": lax.rem(j + 1, n_tm)},
            device_id_type=MESH,
        )

    def back(hop, p):
        first, rows = BACK[p]
        mine, place = xo.at[0, pl.ds(1 + first, rows)], xr.at[0, pl.ds(1 + first, rows)]
        line = (mine, hop1.at[p, pl.ds(0, rows)], hop2.at[p, pl.ds(0, rows)], place)
        return pltpu.make_async_remote_copy(
            src_ref=line[hop], dst_ref=line[hop + 1],
            send_sem=back_send.at[len(BACK) * hop + p], recv_sem=back_recv.at[len(BACK) * hop + p],
            device_id={"tm": lax.rem(j + n_tm - 1, n_tm)}, device_id_type=MESH,
        )

    def pass_back(hop, p):
        back(hop - 1, p).wait_recv()
        back(hop, p).start()

    def edge(i, src, dst, ssem, rsem):
        return pltpu.make_async_remote_copy(
            src_ref=src, dst_ref=dst, send_sem=ssem, recv_sem=rsem,
            device_id={"rows": lax.rem(r + (n_rows - 1 if i == 0 else 1), n_rows)},
            device_id_type=MESH,
        )

    def own_edge(i):
        return edge(
            i, xo.at[:, 1 if i == 0 else height], xo.at[:, height + 1 if i == 0 else 0],
            halo_send.at[i], halo_recv.at[i],
        )

    def fwd_edge(f, i):
        return edge(
            i, xr.at[f, 1 if i == 0 else height], xr.at[f, height + 1 if i == 0 else 0],
            fwd_send.at[2 * f + i], fwd_recv.at[2 * f + i],
        )

    recvs_on, up_on, down_on = j > 0, r > 0, r < n_rows - 1

    a = lax.broadcasted_iota(jnp.int32, (ch, ch), 0)
    b = lax.broadcasted_iota(jnp.int32, (ch, ch), 1)
    group_of = lambda i: lax.shift_right_logical(i * 43691, 19)
    ind[...] = jnp.where(group_of(a) == group_of(b), 1.0, 0.0).astype(BF16)

    def over_group(v):
        v = jnp.broadcast_to(v, (8, ch))
        hi = v.astype(BF16).astype(F32)
        mid = (v - hi).astype(BF16).astype(F32)
        lo = v - hi - mid
        parts = jnp.concatenate([hi, mid, lo, jnp.zeros_like(v)], axis=0).astype(BF16)
        got = jnp.dot(parts, ind[...], preferred_element_type=F32)
        return got[0:1] + (got[8:9] + got[16:17])

    load.wait()
    pixels = 1.0 * frames * height * width

    def fold(v):
        return jnp.sum(v.reshape(-1, 32, ch), axis=0)

    def over_rows(v):
        return jnp.sum(v, axis=0, keepdims=True)

    pivot = over_rows(fold(xo[0, 1].astype(F32))) * (1.0 / width)

    def sums(i, acc):
        first, second = acc
        d = xo[lax.div(i, height), 1 + lax.rem(i, height)].astype(F32) - pivot
        return first + fold(d), second + fold(d * d)

    zero = jnp.zeros((32, ch), F32)
    first, second = lax.fori_loop(0, frames * height, sums, (zero, zero))
    first, second = over_rows(first), over_rows(second)
    mean = pivot + first * (1.0 / pixels)
    square = second - first * (first * (1.0 / pixels))

    top = lax.broadcasted_iota(jnp.int32, (2, ch), 0) == 0

    def exchange(mean, square, count, peers, outbox, inbox, ssem, rsem, between):
        size = len(peers) + 1
        outbox[...] = jnp.where(top, mean, square)
        copies = [
            pltpu.make_async_remote_copy(
                src_ref=outbox, dst_ref=inbox.at[d], send_sem=ssem.at[d], recv_sem=rsem.at[d],
                device_id=peers[d], device_id_type=MESH,
            )
            for d in range(size - 1)
        ]
        for c in copies:
            c.start()
        between()
        for c in copies:
            c.wait()
        got = [inbox[d] for d in range(size - 1)]
        means = [mean] + [g[0:1] for g in got]
        whole = sum(means) * (1.0 / size)
        squares = square + sum(g[1:2] for g in got)
        for m in means:
            squares = squares + count * ((m - whole) * (m - whole))
        return whole, squares

    def frames_away():
        for p in range(len(BACK)):
            back(0, p).start()
        for i in range(len(PIECES)):
            bulk(i).start()
        own_edge(0).start()
        own_edge(1).start()

    pl.semaphore_wait(barrier, len(tm_peers) + len(row_peers))
    mean, square = exchange(
        mean, square, pixels, tm_peers, tm_out, tm_in, tm_send, tm_recv, frames_away
    )
    mean, square = exchange(
        mean, square, pixels * n_tm, row_peers, row_out, row_in, row_send, row_recv, lambda: None
    )
    pass_back(1, 0)
    channel_mean = mean
    mean = over_group(channel_mean) * (1.0 / per_group)
    off = channel_mean - mean
    square = over_group(square + (pixels * n_tm * n_rows) * (off * off))
    inverse = lax.rsqrt(square * (1.0 / cells) + EPS)
    for c in vectors:
        c.wait()
    scale = 0.5 * (inverse * gv[pl.ds(0, ch)].reshape(1, ch))
    shift = 0.5 * gv[pl.ds(ch, ch)].reshape(1, ch)

    def kept(on):
        return jnp.where(on, scale, 0.0), jnp.where(on, shift, 0.0)

    factors = [kept(up_on), (scale, shift), kept(down_on)]

    def normalize(src, f, dst, row):
        by, plus = factors[0 if row == 0 else 2 if row == height + 1 else 1]
        h = (src[f, row].astype(F32) - mean) * by + plus
        dst[row] = (h + h * jnp.tanh(h)).astype(BF16)

    def norms(src, f, dst, rows):
        return [functools.partial(normalize, src, f, dst, row) for row in rows]

    cut = 4 * 256

    def lhs_of(used, first, rows):
        return jnp.concatenate(
            [
                act[pl.ds(first + kh, rows)].reshape(rows * width, ch)
                for act in used
                for kh in range(3)
            ],
            axis=1,
        )

    def put(t, first, rows, lo, got, add):
        got = got.reshape(rows, width, got.shape[1])
        at = (t, pl.ds(first, rows), slice(None), pl.ds(lo, got.shape[2]))
        z[at] = z[at] + got if add else got

    def weights(kt, n, lo, size):
        return wv[pl.ds(kt, n), :, :, pl.ds(lo, size)].reshape(n * 3 * ch, size)

    def main(t, used, kt, first, rows, add):
        def tile(lo):
            got = jnp.dot(
                lhs_of(used, first, rows), weights(kt, len(used), lo, 256), preferred_element_type=F32
            )
            put(t, first, rows, lo, got, add)

        return [functools.partial(tile, lo) for lo in range(0, cut, 256)]

    def pair(act, kts, first, rows, add):
        def tile():
            rhs = jnp.concatenate([weights(kt, 1, cut, 128) for kt in kts], axis=1)
            got = jnp.dot(lhs_of((act,), first, rows), rhs, preferred_element_type=F32)
            put(0, first, rows, cut, got[:, :128], add)
            put(1, first, rows, cut, got[:, 128:], add)

        return [tile]

    def single(t, act, kt, first, rows):
        def tile():
            got = jnp.dot(
                lhs_of((act,), first, rows), weights(kt, 1, cut, 128), preferred_element_type=F32
            )
            put(t, first, rows, cut, got, True)

        return [tile]

    def some(first, rows, khs):
        def tile(lo):
            n = min(256, 3 * ch - lo)
            lhs = jnp.concatenate(
                [act_a[pl.ds(first + kh, rows)].reshape(rows * width, ch) for kh in khs], axis=1
            )
            rhs = jnp.concatenate([wv[0, kh, :, pl.ds(lo, n)] for kh in khs], axis=0)
            put(0, first, rows, lo, jnp.dot(lhs, rhs, preferred_element_type=F32), True)

        return [functools.partial(tile, lo) for lo in range(0, 3 * ch, 256)]

    def run(tiles, side=()):
        done = 0
        for i, tile in enumerate(tiles):
            tile()
            upto = len(side) * (i + 1) // len(tiles)
            for task in side[done:upto]:
                task()
            done = upto

    wi = lax.broadcasted_iota(jnp.int32, (width, ch), 0)

    def finish(t, h):
        left = pltpu.roll(z[t, h, :, 0:ch], 1, 0)
        right = pltpu.roll(z[t, h, :, 2 * ch : 3 * ch], width - 1, 0)
        conv = z[t, h, :, ch : 2 * ch]
        conv = conv + jnp.where(wi == 0, 0.0, left) + jnp.where(wi == width - 1, 0.0, right)
        cbias = gv[pl.ds(2 * ch, ch)].reshape(1, ch)
        out[0, t, h] = (xo[t, h + 1].astype(F32) + conv + cbias).astype(BF16)

    def finishes(t, first, rows):
        return [functools.partial(finish, t, h) for h in range(first, first + rows)]

    def forward(f):
        for i, p in enumerate(PIECES):
            if p in ((f, 0, 1), (f, height - 1, 1)):
                bulk(i).wait_recv()
        fwd_edge(f, 0).start()
        fwd_edge(f, 1).start()

    def edges_in(f):
        fwd_edge(f, 0).wait_recv()
        fwd_edge(f, 1).wait_recv()

    low, high = range(0, half + 2), range(half + 2, height + 2)
    forward(1)
    own_edge(0).wait_recv()
    own_edge(1).wait_recv()

    run(norms(xo, 0, act_c, low))
    for c in wloads:
        c.wait()
    run(
        main(0, (act_c,), 2, 0, half, False) + pair(act_c, (2, 1), 0, half, False),
        norms(xo, 1, act_d, low),
    )
    run(
        main(1, (act_c, act_d), 1, 0, half, False) + single(1, act_d, 2, 0, half),
        norms(xo, 0, act_c, high) + norms(xo, 1, act_d, high),
    )
    pass_back(1, 1)
    pass_back(1, 2)
    edges_in(1)
    run(
        pair(act_c, (2, 1), half, half, False)
        + main(1, (act_c, act_d), 1, half, half, False)
        + single(1, act_d, 2, half, half),
        norms(xr, 1, act_b, (0, 1, 8, 9)),
    )
    pass_back(2, 0)

    @pl.when(recvs_on)
    def _():
        bulk(2).wait_recv()
        run(norms(xr, 1, act_b, (2, 3, 4, 5)))
        run(
            main(0, (act_b,), 1, 0, half, True)
            + main(1, (act_b,), 0, 0, half, True)
            + pair(act_b, (1, 0), 0, half, True)
        )
        pass_back(2, 1)
        pass_back(2, 2)
        bulk(3).wait_recv()
        run(norms(xr, 1, act_b, (6, 7)))
        run(
            main(0, (act_b, act_c), 1, half, half, False) + main(1, (act_b,), 0, half, half, True),
            finishes(1, 0, half),
        )
        forward(0)
        back(2, 0).wait_recv()
        run(pair(act_b, (1, 0), half, half, True), norms(xr, 0, act_a, (1, 2, 3)))
        run(
            some(1, 1, (0, 1, 2)) + some(0, 1, (1, 2)) + some(2, 1, (0, 1)) + some(3, 1, (0,)),
            norms(xr, 0, act_a, (8,)) + finishes(1, half, half),
        )
        bulk(6).wait_recv()
        back(2, 1).wait_recv()
        run(norms(xr, 0, act_a, (4,)))
        run(
            some(2, 1, (2,)) + some(6, 1, (2,)) + some(3, 1, (1, 2)) + some(4, 1, (0, 1))
            + some(5, 1, (0,)) + some(7, 1, (1,)),
            norms(xr, 0, act_a, (5,)) + finishes(0, 1, 2),
        )
        bulk(7).wait_recv()
        back(2, 2).wait_recv()
        edges_in(0)
        run(norms(xr, 0, act_a, (6,)))
        run(some(4, 1, (2,)), norms(xr, 0, act_a, (7, 0, 9)) + finishes(0, 3, 1))
        run(some(5, 1, (1, 2)), finishes(0, 4, 1))
        run(some(0, 1, (0,)), finishes(0, 5, 1))
        run(some(6, 1, (0, 1)), finishes(0, 0, 1))
        run(some(7, 1, (0, 2)), finishes(0, 6, 1))
        run(finishes(0, 7, 1))

    @pl.when(jnp.logical_not(recvs_on))
    def _():
        run(main(0, (act_c,), 2, half, half, False))
        pass_back(2, 1)
        pass_back(2, 2)
        for t in range(frames):
            run(finishes(t, 0, height))
        for i in range(2, len(PIECES)):
            bulk(i).wait_recv()
        for p in range(len(BACK)):
            back(2, p).wait_recv()

    for i in range(len(PIECES)):
        bulk(i).wait_send()
    for hop in range(3):
        for p in range(len(BACK)):
            back(hop, p).wait_send()
    for i in range(2):
        own_edge(i).wait_send()
        fwd_edge(1, i).wait_send()

        @pl.when(recvs_on)
        def _():
            fwd_edge(0, i).wait_send()


def shards(inputs, norm_gain, norm_bias, conv_weight, conv_bias):
    clips, frames, height, width, ch = inputs.shape
    n_tm, n_rows = lax.axis_size("tm"), lax.axis_size("rows")
    per_group = ch // GROUPS
    cells = 1.0 * clips * frames * height * width * per_group * n_tm * n_rows
    hbm = pl.BlockSpec(memory_space=pltpu.HBM)
    dma = lambda n: pltpu.SemaphoreType.DMA((n,))
    act = pltpu.VMEM((height + 2, width, ch), BF16)
    hop = pltpu.VMEM((len(BACK), BACK[0][1], width, ch), BF16)
    return pl.pallas_call(
        functools.partial(kernel, cells, per_group),
        out_shape=jax.ShapeDtypeStruct(inputs.shape, BF16),
        in_specs=[hbm] * 5,
        out_specs=pl.BlockSpec(memory_space=pltpu.VMEM),
        scratch_shapes=[
            pltpu.VMEM((frames, height + 2, width, ch), BF16),
            pltpu.VMEM((2, height + 2, width, ch), BF16),
            act,
            act,
            act,
            act,
            pltpu.VMEM((3, 3, ch, 3 * ch), BF16),
            pltpu.VMEM((frames, height, width, 3 * ch), F32),
            pltpu.VMEM((ch, ch), BF16),
            pltpu.VMEM((2, ch), F32),
            pltpu.VMEM((n_tm - 1, 2, ch), F32),
            pltpu.VMEM((2, ch), F32),
            pltpu.VMEM((n_rows - 1, 2, ch), F32),
            hop,
            hop,
            pltpu.VMEM((3 * ch,), F32),
            pltpu.SemaphoreType.DMA,
            dma(3),
            dma(3),
            dma(len(PIECES)),
            dma(len(PIECES)),
            dma(3 * len(BACK)),
            dma(3 * len(BACK)),
            dma(2),
            dma(2),
            dma(4),
            dma(4),
            dma(n_tm - 1),
            dma(n_tm - 1),
            dma(n_rows - 1),
            dma(n_rows - 1),
        ],
        compiler_params=pltpu.CompilerParams(
            collective_id=0, has_side_effects=True, vmem_limit_bytes=51 * 1024 * 1024
        ),
    )(
        inputs, *(pltpu.with_memory_space_constraint(v, pltpu.HBM) for v in (norm_gain, norm_bias, conv_bias)), conv_weight
    )


def solution(mesh):
    placed = (P("batch", "tm", "rows", None, None), P(), P(), P(), P())
    return jax.shard_map(
        shards,
        mesh=mesh,
        in_specs=placed,
        out_specs=P("batch", "tm", "rows", None, None),
        check_vma=False,
    )
```

```python
import functools

import jax
import jax.numpy as jnp
from jax import lax
from jax.experimental import pallas as pl
from jax.experimental.pallas import tpu as pltpu
from jax.sharding import PartitionSpec as P

MESH = pl.DeviceIdType.MESH
GROUPS = 32
EPS = 1e-06
F32 = jnp.float32
BF16 = jnp.bfloat16

PIECES = ((1, 0, 1), (1, 7, 1), (1, 1, 4), (1, 5, 2), (0, 0, 1), (0, 7, 1), (0, 3, 1), (0, 5, 1))
BACK = ((1, 2), (4, 1), (6, 1))


def kernel(
    cells, per_group,
    x, gain, bias, cbias, w, out,
    xo, xr, act_a, act_b, act_c, act_d, wv, z, ind, tm_out, tm_in, row_out, row_in, hop1, hop2, gv,
    load_sem, wsem, vec_sem,
    bulk_send, bulk_recv, back_send, back_recv, halo_send, halo_recv, fwd_send, fwd_recv,
    tm_send, tm_recv, row_send, row_recv,
):
    n_tm, n_rows = lax.axis_size("tm"), lax.axis_size("rows")
    j, r = lax.axis_index("tm"), lax.axis_index("rows")
    frames, height, width, ch = xo.shape[0], xo.shape[1] - 2, xo.shape[2], xo.shape[3]
    half = height // 2

    load = pltpu.make_async_copy(x.at[0], xo.at[:, 1 : height + 1], load_sem)
    load.start()
    vectors = [
        pltpu.make_async_copy(v, gv.at[pl.ds(i * ch, ch)], vec_sem.at[i])
        for i, v in enumerate((gain, bias, cbias))
    ]
    for c in vectors:
        c.start()
    wloads = [
        pltpu.make_async_copy(w.at[:, :, kw], wv.at[:, :, :, pl.ds(kw * ch, ch)], wsem.at[kw])
        for kw in range(3)
    ]
    for c in wloads:
        c.start()

    barrier = pltpu.get_barrier_semaphore()
    tm_peers = [{"tm": lax.rem(j + d, n_tm)} for d in range(1, n_tm)]
    row_peers = [{"rows": lax.rem(r + d, n_rows)} for d in range(1, n_rows)]
    for peer in tm_peers + row_peers:
        pl.semaphore_signal(barrier, inc=1, device_id=peer, device_id_type=MESH)

    def bulk(i):
        f, first, rows = PIECES[i]
        return pltpu.make_async_remote_copy(
            src_ref=xo.at[f, pl.ds(1 + first, rows)],
            dst_ref=xr.at[f, pl.ds(1 + first, rows)],
            send_sem=bulk_send.at[i],
            recv_sem=bulk_recv.at[i],
            device_id={"tm": lax.rem(j + 1, n_tm)},
            device_id_type=MESH,
        )

    def back(hop, p):
        first, rows = BACK[p]
        mine, place = xo.at[0, pl.ds(1 + first, rows)], xr.at[0, pl.ds(1 + first, rows)]
        line = (mine, hop1.at[p, pl.ds(0, rows)], hop2.at[p, pl.ds(0, rows)], place)
        return pltpu.make_async_remote_copy(
            src_ref=line[hop], dst_ref=line[hop + 1],
            send_sem=back_send.at[len(BACK) * hop + p], recv_sem=back_recv.at[len(BACK) * hop + p],
            device_id={"tm": lax.rem(j + n_tm - 1, n_tm)}, device_id_type=MESH,
        )

    def pass_back(hop, p):
        back(hop - 1, p).wait_recv()
        back(hop, p).start()

    def edge(i, src, dst, ssem, rsem):
        return pltpu.make_async_remote_copy(
            src_ref=src, dst_ref=dst, send_sem=ssem, recv_sem=rsem,
            device_id={"rows": lax.rem(r + (n_rows - 1 if i == 0 else 1), n_rows)},
            device_id_type=MESH,
        )

    def own_edge(i):
        return edge(
            i, xo.at[:, 1 if i == 0 else height], xo.at[:, height + 1 if i == 0 else 0],
            halo_send.at[i], halo_recv.at[i],
        )

    def fwd_edge(f, i):
        return edge(
            i, xr.at[f, 1 if i == 0 else height], xr.at[f, height + 1 if i == 0 else 0],
            fwd_send.at[2 * f + i], fwd_recv.at[2 * f + i],
        )

    recvs_on, up_on, down_on = j > 0, r > 0, r < n_rows - 1

    a = lax.broadcasted_iota(jnp.int32, (ch, ch), 0)
    b = lax.broadcasted_iota(jnp.int32, (ch, ch), 1)
    group_of = lambda i: lax.shift_right_logical(i * 43691, 19)
    ind[...] = jnp.where(group_of(a) == group_of(b), 1.0, 0.0).astype(BF16)

    def over_group(v):
        v = jnp.broadcast_to(v, (8, ch))
        hi = v.astype(BF16).astype(F32)
        mid = (v - hi).astype(BF16).astype(F32)
        lo = v - hi - mid
        parts = jnp.concatenate([hi, mid, lo, jnp.zeros_like(v)], axis=0).astype(BF16)
        got = jnp.dot(parts, ind[...], preferred_element_type=F32)
        return got[0:1] + (got[8:9] + got[16:17])

    load.wait()
    pixels = 1.0 * frames * height * width

    def fold(v):
        return jnp.sum(v.reshape(-1, 32, ch), axis=0)

    def over_rows(v):
        return jnp.sum(v, axis=0, keepdims=True)

    pivot = over_rows(fold(xo[0, 1].astype(F32))) * (1.0 / width)

    def sums(i, acc):
        first, second = acc
        d = xo[lax.div(i, height), 1 + lax.rem(i, height)].astype(F32) - pivot
        return first + fold(d), second + fold(d * d)

    zero = jnp.zeros((32, ch), F32)
    first, second = lax.fori_loop(0, frames * height, sums, (zero, zero))
    first, second = over_rows(first), over_rows(second)
    mean = pivot + first * (1.0 / pixels)
    square = second - first * (first * (1.0 / pixels))

    top = lax.broadcasted_iota(jnp.int32, (2, ch), 0) == 0

    def exchange(mean, square, count, peers, outbox, inbox, ssem, rsem, between):
        size = len(peers) + 1
        outbox[...] = jnp.where(top, mean, square)
        copies = [
            pltpu.make_async_remote_copy(
                src_ref=outbox, dst_ref=inbox.at[d], send_sem=ssem.at[d], recv_sem=rsem.at[d],
                device_id=peers[d], device_id_type=MESH,
            )
            for d in range(size - 1)
        ]
        for c in copies:
            c.start()
        between()
        for c in copies:
            c.wait()
        got = [inbox[d] for d in range(size - 1)]
        means = [mean] + [g[0:1] for g in got]
        whole = sum(means) * (1.0 / size)
        squares = square + sum(g[1:2] for g in got)
        for m in means:
            squares = squares + count * ((m - whole) * (m - whole))
        return whole, squares

    def frames_away():
        for p in range(len(BACK)):
            back(0, p).start()
        for i in range(len(PIECES)):
            bulk(i).start()
        own_edge(0).start()
        own_edge(1).start()

    pl.semaphore_wait(barrier, len(tm_peers) + len(row_peers))
    mean, square = exchange(
        mean, square, pixels, tm_peers, tm_out, tm_in, tm_send, tm_recv, frames_away
    )
    mean, square = exchange(
        mean, square, pixels * n_tm, row_peers, row_out, row_in, row_send, row_recv, lambda: None
    )
    pass_back(1, 0)
    channel_mean = mean
    mean = over_group(channel_mean) * (1.0 / per_group)
    off = channel_mean - mean
    square = over_group(square + (pixels * n_tm * n_rows) * (off * off))
    inverse = lax.rsqrt(square * (1.0 / cells) + EPS)
    for c in vectors:
        c.wait()
    scale = 0.5 * (inverse * gv[pl.ds(0, ch)].reshape(1, ch))
    shift = 0.5 * gv[pl.ds(ch, ch)].reshape(1, ch)

    def kept(on):
        return jnp.where(on, scale, 0.0), jnp.where(on, shift, 0.0)

    factors = [kept(up_on), (scale, shift), kept(down_on)]

    def normalize(src, f, dst, row):
        by, plus = factors[0 if row == 0 else 2 if row == height + 1 else 1]
        h = (src[f, row].astype(F32) - mean) * by + plus
        dst[row] = (h + h * jnp.tanh(h)).astype(BF16)

    def norms(src, f, dst, rows):
        return [functools.partial(normalize, src, f, dst, row) for row in rows]

    cut = 4 * 256

    def lhs_of(used, first, rows):
        return jnp.concatenate(
            [
                act[pl.ds(first + kh, rows)].reshape(rows * width, ch)
                for act in used
                for kh in range(3)
            ],
            axis=1,
        )

    def put(t, first, rows, lo, got, add):
        got = got.reshape(rows, width, got.shape[1])
        at = (t, pl.ds(first, rows), slice(None), pl.ds(lo, got.shape[2]))
        z[at] = z[at] + got if add else got

    def weights(kt, n, lo, size):
        return wv[pl.ds(kt, n), :, :, pl.ds(lo, size)].reshape(n * 3 * ch, size)

    def main(t, used, kt, first, rows, add):
        def tile(lo):
            got = jnp.dot(
                lhs_of(used, first, rows), weights(kt, len(used), lo, 256), preferred_element_type=F32
            )
            put(t, first, rows, lo, got, add)

        return [functools.partial(tile, lo) for lo in range(0, cut, 256)]

    def pair(act, kts, first, rows, add):
        def tile():
            rhs = jnp.concatenate([weights(kt, 1, cut, 128) for kt in kts], axis=1)
            got = jnp.dot(lhs_of((act,), first, rows), rhs, preferred_element_type=F32)
            put(0, first, rows, cut, got[:, :128], add)
            put(1, first, rows, cut, got[:, 128:], add)

        return [tile]

    def single(t, act, kt, first, rows):
        def tile():
            got = jnp.dot(
                lhs_of((act,), first, rows), weights(kt, 1, cut, 128), preferred_element_type=F32
            )
            put(t, first, rows, cut, got, True)

        return [tile]

    def some(first, rows, khs):
        def tile(lo):
            n = min(256, 3 * ch - lo)
            lhs = jnp.concatenate(
                [act_a[pl.ds(first + kh, rows)].reshape(rows * width, ch) for kh in khs], axis=1
            )
            rhs = jnp.concatenate([wv[0, kh, :, pl.ds(lo, n)] for kh in khs], axis=0)
            put(0, first, rows, lo, jnp.dot(lhs, rhs, preferred_element_type=F32), True)

        return [functools.partial(tile, lo) for lo in range(0, 3 * ch, 256)]

    def run(tiles, side=()):
        done = 0
        for i, tile in enumerate(tiles):
            tile()
            upto = len(side) * (i + 1) // len(tiles)
            for task in side[done:upto]:
                task()
            done = upto

    wi = lax.broadcasted_iota(jnp.int32, (width, ch), 0)

    def finish(t, h):
        left = pltpu.roll(z[t, h, :, 0:ch], 1, 0)
        right = pltpu.roll(z[t, h, :, 2 * ch : 3 * ch], width - 1, 0)
        conv = z[t, h, :, ch : 2 * ch]
        conv = conv + jnp.where(wi == 0, 0.0, left) + jnp.where(wi == width - 1, 0.0, right)
        cbias = gv[pl.ds(2 * ch, ch)].reshape(1, ch)
        out[0, t, h] = (xo[t, h + 1].astype(F32) + conv + cbias).astype(BF16)

    def finishes(t, first, rows):
        return [functools.partial(finish, t, h) for h in range(first, first + rows)]

    def forward(f):
        for i, p in enumerate(PIECES):
            if p in ((f, 0, 1), (f, height - 1, 1)):
                bulk(i).wait_recv()
        fwd_edge(f, 0).start()
        fwd_edge(f, 1).start()

    def edges_in(f):
        fwd_edge(f, 0).wait_recv()
        fwd_edge(f, 1).wait_recv()

    def early_sends():
        for i in range(len(PIECES) - 1):
            bulk(i).wait_send()
        for hop in range(2):
            for p in range(len(BACK)):
                back(hop, p).wait_send()
        for i in range(2):
            own_edge(i).wait_send()
            fwd_edge(1, i).wait_send()

    low, high = range(0, half + 2), range(half + 2, height + 2)
    forward(1)
    own_edge(0).wait_recv()
    own_edge(1).wait_recv()

    run(norms(xo, 0, act_c, low))
    for c in wloads:
        c.wait()
    run(
        main(0, (act_c,), 2, 0, half, False) + pair(act_c, (2, 1), 0, half, False),
        norms(xo, 1, act_d, low),
    )
    run(
        main(1, (act_c, act_d), 1, 0, half, False) + single(1, act_d, 2, 0, half),
        norms(xo, 0, act_c, high) + norms(xo, 1, act_d, high),
    )
    pass_back(1, 1)
    pass_back(1, 2)
    edges_in(1)
    run(
        pair(act_c, (2, 1), half, half, False)
        + main(1, (act_c, act_d), 1, half, half, False)
        + single(1, act_d, 2, half, half),
        norms(xr, 1, act_b, (0, 1, 8, 9)),
    )
    pass_back(2, 0)

    @pl.when(recvs_on)
    def _():
        bulk(2).wait_recv()
        run(norms(xr, 1, act_b, (2, 3, 4, 5)))
        run(
            main(0, (act_b,), 1, 0, half, True)
            + main(1, (act_b,), 0, 0, half, True)
            + pair(act_b, (1, 0), 0, half, True)
        )
        pass_back(2, 1)
        pass_back(2, 2)
        bulk(3).wait_recv()
        run(norms(xr, 1, act_b, (6, 7)))
        run(
            main(0, (act_b, act_c), 1, half, half, False) + main(1, (act_b,), 0, half, half, True),
            finishes(1, 0, half),
        )
        forward(0)
        back(2, 0).wait_recv()
        run(pair(act_b, (1, 0), half, half, True), norms(xr, 0, act_a, (1, 2, 3)))
        run(
            some(1, 1, (0, 1, 2)) + some(0, 1, (1, 2)) + some(2, 1, (0, 1)) + some(3, 1, (0,)),
            norms(xr, 0, act_a, (8,)) + finishes(1, half, half),
        )
        bulk(6).wait_recv()
        back(2, 1).wait_recv()
        run(norms(xr, 0, act_a, (4,)))
        run(
            some(2, 1, (2,)) + some(6, 1, (2,)) + some(3, 1, (1, 2)) + some(4, 1, (0, 1))
            + some(5, 1, (0,)) + some(7, 1, (1,)),
            norms(xr, 0, act_a, (5,)) + finishes(0, 1, 2),
        )
        early_sends()
        bulk(7).wait_recv()
        back(2, 2).wait_recv()
        edges_in(0)
        run(norms(xr, 0, act_a, (6,)))
        run(some(4, 1, (2,)), norms(xr, 0, act_a, (7, 0, 9)) + finishes(0, 3, 1))
        run(some(5, 1, (1, 2)), finishes(0, 4, 1))
        run(some(0, 1, (0,)), finishes(0, 5, 1))
        run(some(6, 1, (0, 1)), finishes(0, 0, 1))
        run(some(7, 1, (0, 2)), finishes(0, 6, 1))
        run(finishes(0, 7, 1))

    @pl.when(jnp.logical_not(recvs_on))
    def _():
        run(main(0, (act_c,), 2, half, half, False))
        pass_back(2, 1)
        pass_back(2, 2)
        for t in range(frames):
            run(finishes(t, 0, height))
        early_sends()
        for i in range(2, len(PIECES)):
            bulk(i).wait_recv()
        for p in range(len(BACK)):
            back(2, p).wait_recv()

    bulk(len(PIECES) - 1).wait_send()
    for p in range(len(BACK)):
        back(2, p).wait_send()

    @pl.when(recvs_on)
    def _():
        for i in range(2):
            fwd_edge(0, i).wait_send()


def shards(inputs, norm_gain, norm_bias, conv_weight, conv_bias):
    clips, frames, height, width, ch = inputs.shape
    n_tm, n_rows = lax.axis_size("tm"), lax.axis_size("rows")
    per_group = ch // GROUPS
    cells = 1.0 * clips * frames * height * width * per_group * n_tm * n_rows
    hbm = pl.BlockSpec(memory_space=pltpu.HBM)
    dma = lambda n: pltpu.SemaphoreType.DMA((n,))
    act = pltpu.VMEM((height + 2, width, ch), BF16)
    hop = pltpu.VMEM((len(BACK), BACK[0][1], width, ch), BF16)
    return pl.pallas_call(
        functools.partial(kernel, cells, per_group),
        out_shape=jax.ShapeDtypeStruct(inputs.shape, BF16),
        in_specs=[hbm] * 5,
        out_specs=pl.BlockSpec(memory_space=pltpu.VMEM),
        scratch_shapes=[
            pltpu.VMEM((frames, height + 2, width, ch), BF16),
            pltpu.VMEM((2, height + 2, width, ch), BF16),
            act,
            act,
            act,
            act,
            pltpu.VMEM((3, 3, ch, 3 * ch), BF16),
            pltpu.VMEM((frames, height, width, 3 * ch), F32),
            pltpu.VMEM((ch, ch), BF16),
            pltpu.VMEM((2, ch), F32),
            pltpu.VMEM((n_tm - 1, 2, ch), F32),
            pltpu.VMEM((2, ch), F32),
            pltpu.VMEM((n_rows - 1, 2, ch), F32),
            hop,
            hop,
            pltpu.VMEM((3 * ch,), F32),
            pltpu.SemaphoreType.DMA,
            dma(3),
            dma(3),
            dma(len(PIECES)),
            dma(len(PIECES)),
            dma(3 * len(BACK)),
            dma(3 * len(BACK)),
            dma(2),
            dma(2),
            dma(4),
            dma(4),
            dma(n_tm - 1),
            dma(n_tm - 1),
            dma(n_rows - 1),
            dma(n_rows - 1),
        ],
        compiler_params=pltpu.CompilerParams(
            collective_id=0, has_side_effects=True, vmem_limit_bytes=51 * 1024 * 1024
        ),
    )(
        inputs, *(pltpu.with_memory_space_constraint(v, pltpu.HBM) for v in (norm_gain, norm_bias, conv_bias)), conv_weight
    )


def solution(mesh):
    placed = (P("batch", "tm", "rows", None, None), P(), P(), P(), P())
    return jax.shard_map(
        shards,
        mesh=mesh,
        in_specs=placed,
        out_specs=P("batch", "tm", "rows", None, None),
        check_vma=False,
    )
```
